32 devices in a mesh: grp: 2 (over x), spec: 16 (over z, y, core).
Axes of the slice: x: 2, y: 2, z: 4, core: 2. Of those that a mesh axis runs over, the one named last changes fastest.
Arguments:
- spectrum: float32 [3072, 1536], P(('grp', 'spec')), parts along dimension 0, may hold values from 0.05 to 5
- sea_mask: int32 [1536], replicated, may hold values from 0 to 1, as said below
- wind_speed: float32 [3072], P('grp'), parts along dimension 0, may hold values from 0.3 to 3
- wind_angle: float32 [3072], P('grp'), parts along dimension 0, may hold values from -3.140625 to 3.140625
Outputs:
- new_spectrum: float32 [3072, 1536], P(('grp', 'spec')), parts along dimension 0
- wave_height: float32 [3072], P(('grp', 'spec')), parts along dimension 0
- mean_height: float32 [2], P('grp'), parts along dimension 0
The draws below stay inside these ranges and needn't reach their ends.
There are 2 independent parts, one for each index of `grp`. The reference program is written for one: setup_inputs(seed, part) draws one part's arguments, and reference() takes and returns one part's arrays. A program takes and returns all parts, laid end to end along the dimension named above; an argument that names none is the same for every part. Nothing has to cross between parts.
Inputs may be any that keep to these rules, and one draw needn't show every extreme that they name: `sea_mask`: exactly 1024 cells are sea.
All inputs are finite; a program needn't handle non-finite values.
Results may differ from the reference program's by a relative error of at most 0.00002.
Values sent between devices are 32-bit elements; how exact they have to be, the bound alone decides.
A program may use at most 64 MiB of HBM per device.

```python
import math
import jax
import jax.numpy as jnp
from jax import lax

NF = 48
ND = 32
NLON = 384
ADV_STEPS = 2
PTS_DEV = 96
BINS = 1536
CELLS = 1536
NLAT = 4
SEA = 1024
N_SPEC = 16


def draw_sea_mask(key, part):
    coarse_key, fine_key = jax.random.split(jax.random.fold_in(key, 17))
    block_rows = (NLAT + 7) // 8
    block_cols = (NLON + 7) // 8
    coarse = jax.random.randint(coarse_key, (block_rows, block_cols), 0, 64)
    fine = jax.random.randint(fine_key, (NLAT, NLON), 0, 16)
    row_ids = jnp.arange(NLAT, dtype=jnp.int32) // 8
    col_ids = jnp.arange(NLON, dtype=jnp.int32) // 8
    spread = coarse[row_ids][:, col_ids] * 16 + fine
    scores = spread.reshape(-1) * CELLS + jnp.arange(CELLS, dtype=jnp.int32)
    order = jnp.argsort(scores, stable=True)
    chosen = order[:SEA]
    return jnp.zeros((CELLS,), jnp.int32).at[chosen].set(1)


def levels(stream_key, shape, cuts, least, top_value):
    def one(position, blocks):
        draws = jax.random.uniform(jax.random.fold_in(jax.random.fold_in(stream_key, 6), position), (blocks,), jnp.float32, least / len(cuts), top_value / len(cuts))
        return jnp.repeat(jnp.exp(draws), shape[position] // blocks).reshape((-1,) + (1,) * (len(shape) - position - 1))

    factor_of = one(*cuts[0])
    for cut in cuts[1:]:
        factor_of = factor_of * one(*cut)
    return factor_of


def setup_inputs(seed: int = 0, part: int = 0) -> dict:
    key_of = jax.random.split(jax.random.key(seed), 5)
    part_splits = jax.random.split(jax.random.fold_in(key_of[4], part), 5)
    spectrum = jnp.clip(jnp.exp(math.log(5.0) - 4.6051702 * jax.random.uniform(part_splits[0], (BINS, CELLS), jnp.float32) ** levels(part_splits[0], (BINS, CELLS), ((0, 16),), -0.2, 0.2)), 0.05, 5.0)
    sea_mask = draw_sea_mask(jax.random.fold_in(key_of[4], 71), part)
    wind_speed = jnp.clip(jnp.exp(jax.random.uniform(part_splits[2], (CELLS,), jnp.float32, math.log(0.3), math.log(3.0))), 0.3, 3.0)
    wind_angle = jnp.clip(jax.random.uniform(part_splits[3], (CELLS,), jnp.float32, -3.140625, 3.140625), -3.140625, 3.140625)
    return {"spectrum": spectrum, "sea_mask": sea_mask, "wind_speed": wind_speed, "wind_angle": wind_angle}


def upwind_step(energy, courant_x, courant_y, sea_grid):
    west_cell = jnp.roll(energy, 1, axis=2)
    east_cell = jnp.roll(energy, -1, axis=2)
    edge_row = jnp.zeros_like(energy[:, :1])
    south_cell = jnp.concatenate([edge_row, energy[:, :-1]], axis=1)
    north_cell = jnp.concatenate([energy[:, 1:], edge_row], axis=1)
    updated = energy - jnp.maximum(courant_x, 0.0) * (energy - west_cell) - jnp.minimum(courant_x, 0.0) * (east_cell - energy) - jnp.maximum(courant_y, 0.0) * (energy - south_cell) - jnp.minimum(courant_y, 0.0) * (north_cell - energy)
    return updated * sea_grid

def courant_numbers(freq_index, dir_index, lat_count, dir_count):
    speed = 0.2 * jnp.exp(-math.log(1.1) * freq_index)
    heading = 2.0 * math.pi * (dir_index + 0.5) / dir_count
    rows = jnp.arange(lat_count, dtype=jnp.float32)
    latitude = (-75.0 + 150.0 * (rows + 0.5) / lat_count) * (math.pi / 180.0)
    courant_x = (speed * jnp.cos(heading))[:, None, None] / jnp.cos(latitude)[None, :, None]
    courant_y = (speed * jnp.sin(heading))[:, None, None]
    return (courant_x, courant_y)

def shift_freq(values, amount):
    if amount > 0:
        filler = jnp.zeros_like(values[:amount])
        return jnp.concatenate([filler, values[:-amount]], axis=0)
    filler = jnp.zeros_like(values[:-amount])
    return jnp.concatenate([values[-amount:], filler], axis=0)

def source_terms(energy, speed, angle):
    freq_count = energy.shape[0]
    dir_count = energy.shape[1]
    freq_ids = jnp.arange(freq_count, dtype=jnp.float32)
    frequency = jnp.exp(math.log(1.1) * (freq_ids - freq_count // 2))[:, None, None]
    heading = (2.0 * math.pi * (jnp.arange(dir_count, dtype=jnp.float32) + 0.5) / dir_count)[None, :, None]
    energy_mean = lax.optimization_barrier(jnp.mean(energy, axis=(0, 1)))
    moment_one = lax.optimization_barrier(jnp.mean(frequency * energy, axis=(0, 1)))
    mean_freq = moment_one / (energy_mean + 1e-06)
    steepness = energy_mean * mean_freq * mean_freq
    breaking = steepness * steepness / (1.0 + steepness * steepness)
    wind_gain = 0.05 * frequency * jnp.maximum(0.0, speed[None, None, :] * frequency * jnp.cos(heading - angle[None, None, :]) - 1.0)
    damping = 0.03 * frequency * breaking[None, None, :]
    valid = ((freq_ids >= 3) & (freq_ids <= freq_count - 3)).astype(jnp.float32)[:, None, None]
    interaction = jnp.zeros_like(energy)
    for mirror in (1, -1):
        plus_bins = shift_freq(jnp.roll(energy, -mirror, axis=1), -2)
        minus_bins = shift_freq(jnp.roll(energy, 3 * mirror, axis=1), 3)
        transfer_rate = 0.001 * valid * (energy * energy * (plus_bins + minus_bins) - 2.0 * energy * plus_bins * minus_bins)
        interaction = interaction - 2.0 * transfer_rate
        interaction = interaction + jnp.roll(shift_freq(transfer_rate, 2), mirror, axis=1)
        interaction = interaction + jnp.roll(shift_freq(transfer_rate, -3), -3 * mirror, axis=1)
    updated = energy + (wind_gain - damping) * energy + interaction
    raw_height = 4.0 * jnp.sqrt(lax.optimization_barrier(jnp.mean(updated, axis=(0, 1))) + 1e-06)
    return (updated, raw_height)

def reference(spectrum, sea_mask, wind_speed, wind_angle):
    sea_float = sea_mask.astype(jnp.float32)
    sea_grid = sea_float.reshape(1, NLAT, NLON)
    bands = (spectrum * sea_float[None, :]).reshape(NF, ND, NLAT, NLON)

    def advect_band(inputs):
        band, freq_value = inputs
        dir_index = jnp.arange(ND, dtype=jnp.float32)
        freq_index = jnp.zeros((ND,), jnp.float32) + freq_value
        courant_x, courant_y = courant_numbers(freq_index, dir_index, NLAT, ND)
        for substep in range(ADV_STEPS):
            band = upwind_step(band, courant_x, courant_y, sea_grid)
        return band
    advected = lax.map(advect_band, (bands, jnp.arange(NF, dtype=jnp.float32)))
    blocks = jnp.moveaxis(advected.reshape(NF, ND, N_SPEC, PTS_DEV), 2, 0)
    speed_blocks = wind_speed.reshape(N_SPEC, PTS_DEV)
    angle_blocks = wind_angle.reshape(N_SPEC, PTS_DEV)

    def block_sources(inputs):
        return source_terms(inputs[0], inputs[1], inputs[2])
    updated, raw_height = lax.map(block_sources, (blocks, speed_blocks, angle_blocks))
    new_spectrum = jnp.moveaxis(updated, 0, 2).reshape(NF * ND, CELLS)
    wave_height = sea_float * raw_height.reshape(CELLS)
    mean_height = (jnp.sum(wave_height) / SEA).reshape(1)
    return (new_spectrum, wave_height, mean_height)
```

```python
import functools
import math

import jax
import jax.numpy as jnp
from jax import lax
from jax.experimental import pallas as pl
from jax.experimental.pallas import tpu as pltpu
from jax.sharding import PartitionSpec as P

NF = 48
ND = 32
NLON = 384
ADV_STEPS = 2
SEA_DEV = 64


def upwind_step(energy, courant_x, courant_y, sea_grid):
    west_cell = jnp.roll(energy, 1, axis=2)
    east_cell = jnp.roll(energy, -1, axis=2)
    edge_row = jnp.zeros_like(energy[:, :1])
    south_cell = jnp.concatenate([edge_row, energy[:, :-1]], axis=1)
    north_cell = jnp.concatenate([energy[:, 1:], edge_row], axis=1)
    updated = (
        energy
        - jnp.maximum(courant_x, 0.0) * (energy - west_cell)
        - jnp.minimum(courant_x, 0.0) * (east_cell - energy)
        - jnp.maximum(courant_y, 0.0) * (energy - south_cell)
        - jnp.minimum(courant_y, 0.0) * (north_cell - energy)
    )
    return updated * sea_grid


def courant_numbers(freq_index, dir_index, lat_count, dir_count):
    speed = 0.2 * jnp.exp(-math.log(1.1) * freq_index)
    heading = 2.0 * math.pi * (dir_index + 0.5) / dir_count
    rows = jnp.arange(lat_count, dtype=jnp.float32)
    latitude = (-75.0 + 150.0 * (rows + 0.5) / lat_count) * (math.pi / 180.0)
    courant_x = (speed * jnp.cos(heading))[:, None, None] / jnp.cos(latitude)[None, :, None]
    courant_y = (speed * jnp.sin(heading))[:, None, None]
    return (courant_x, courant_y)


def shift_freq(values, amount):
    if amount > 0:
        filler = jnp.zeros_like(values[:amount])
        return jnp.concatenate([filler, values[:-amount]], axis=0)
    filler = jnp.zeros_like(values[:-amount])
    return jnp.concatenate([values[-amount:], filler], axis=0)


def source_terms(energy, speed, angle):
    freq_count = energy.shape[0]
    dir_count = energy.shape[1]
    freq_ids = jnp.arange(freq_count, dtype=jnp.float32)
    frequency = jnp.exp(math.log(1.1) * (freq_ids - freq_count // 2))[:, None, None]
    heading = (2.0 * math.pi * (jnp.arange(dir_count, dtype=jnp.float32) + 0.5) / dir_count)[
        None, :, None
    ]
    energy_mean = jnp.mean(energy, axis=(0, 1))
    moment_one = jnp.mean(frequency * energy, axis=(0, 1))
    mean_freq = moment_one / (energy_mean + 1e-06)
    steepness = energy_mean * mean_freq * mean_freq
    breaking = steepness * steepness / (1.0 + steepness * steepness)
    wind_gain = (
        0.05
        * frequency
        * jnp.maximum(
            0.0, speed[None, None, :] * frequency * jnp.cos(heading - angle[None, None, :]) - 1.0
        )
    )
    damping = 0.03 * frequency * breaking[None, None, :]
    valid = ((freq_ids >= 3) & (freq_ids <= freq_count - 3)).astype(jnp.float32)[:, None, None]
    interaction = jnp.zeros_like(energy)
    for mirror in (1, -1):
        plus_bins = shift_freq(jnp.roll(energy, -mirror, axis=1), -2)
        minus_bins = shift_freq(jnp.roll(energy, 3 * mirror, axis=1), 3)
        transfer_rate = (
            0.001
            * valid
            * (energy * energy * (plus_bins + minus_bins) - 2.0 * energy * plus_bins * minus_bins)
        )
        interaction = interaction - 2.0 * transfer_rate
        interaction = interaction + jnp.roll(shift_freq(transfer_rate, 2), mirror, axis=1)
        interaction = interaction + jnp.roll(shift_freq(transfer_rate, -3), -3 * mirror, axis=1)
    updated = energy + (wind_gain - damping) * energy + interaction
    raw_height = 4.0 * jnp.sqrt(jnp.mean(updated, axis=(0, 1)) + 1e-06)
    return (updated, raw_height)


def local(spectrum, sea_mask, wind_speed, wind_angle):
    count = lax.axis_size("spec")
    position = lax.axis_index("spec")
    bins_dev = spectrum.shape[0]
    cells = spectrum.shape[1]
    points = cells // count
    lat_count = cells // NLON
    sea_float = sea_mask.astype(jnp.float32)
    bin_ids = position * bins_dev + jnp.arange(bins_dev, dtype=jnp.int32)
    freq_index = (bin_ids // ND).astype(jnp.float32)
    dir_index = (bin_ids % ND).astype(jnp.float32)
    courant_x, courant_y = courant_numbers(freq_index, dir_index, lat_count, ND)
    sea_grid = sea_float.reshape(1, lat_count, NLON)
    energy = (spectrum * sea_float[None, :]).reshape(bins_dev, lat_count, NLON)
    for substep in range(ADV_STEPS):
        energy = upwind_step(energy, courant_x, courant_y, sea_grid)
    advected = energy.reshape(bins_dev, cells)
    outgoing = advected.reshape(bins_dev, count, points)
    arrived = lax.all_to_all(outgoing, "spec", split_axis=1, concat_axis=0, tiled=True)
    start = position * points
    speed_own = lax.dynamic_slice_in_dim(wind_speed, start, points)
    angle_own = lax.dynamic_slice_in_dim(wind_angle, start, points)
    sea_own = lax.dynamic_slice_in_dim(sea_float, start, points)
    updated, raw_height = source_terms(arrived.reshape(NF, ND, points), speed_own, angle_own)
    wave_height = sea_own * raw_height
    own_total = jnp.zeros((count, 1), jnp.float32) + jnp.sum(wave_height)
    returned, totals = (
        lax.all_to_all(
            updated.reshape(NF * ND, 1, points), "spec", split_axis=0, concat_axis=1, tiled=True
        ),
        lax.all_to_all(own_total, "spec", split_axis=0, concat_axis=1, tiled=True),
    )
    new_spectrum = returned.reshape(bins_dev, cells)
    height_sum = jnp.sum(totals)
    mean_height = (height_sum / (SEA_DEV * count)).reshape(1)
    return (new_spectrum, wave_height, mean_height)


HALO = 5
LANES = 128


def group_size(count, bins_dev, cells):
    size = 4
    if count % size or bins_dev % ND or cells % (size * LANES) or cells % NLON:
        return 0
    if NLON % LANES or bins_dev // ND * size < 2 * HALO or cells % count:
        return 0
    return size


def fused_kernel(
    count, group, aux_ref, spec_ref, out_ref, wave_ref, mean_ref,
    raw, adv, held, done, mom_out, mom_in, wind, acc, sum_out, sum_in,
    load_sem, held_sem, y_sem, up_sem, down_sem, mom_send, mom_recv,
    ret_send, ret_recv, sum_send, sum_recv,
):
    f32 = jnp.float32
    bins_dev, cells = adv.shape
    freq_dev = bins_dev // ND
    freq_group = freq_dev * group
    width = cells // group
    zones = count // group
    lat_count = cells // NLON
    sides = group // 2
    me = lax.axis_index("spec")
    zone, rank = me // group, me % group
    side, core = rank // 2, rank % 2

    def remote(src, dst, send, recv, target):
        return pltpu.make_async_remote_copy(
            src_ref=src, dst_ref=dst, send_sem=send, recv_sem=recv,
            device_id={"spec": target}, device_id_type=pl.DeviceIdType.MESH,
        )

    barrier = pltpu.get_barrier_semaphore()
    for step in range(1, count):
        pl.semaphore_signal(
            barrier, inc=1, device_id={"spec": (me + step) % count},
            device_id_type=pl.DeviceIdType.MESH,
        )
    loads = [
        pltpu.make_async_copy(
            spec_ref.at[pl.ds(f * ND, ND)], raw.at[pl.ds(f * ND, ND)], load_sem.at[f]
        )
        for f in range(freq_dev)
    ]
    for load in loads:
        load.start()

    @pl.when(zone == 0)
    def _():
        held[0:HALO] = jnp.zeros((HALO, ND, width), f32)

    @pl.when(zone == zones - 1)
    def _():
        held[HALO + freq_group :] = jnp.zeros((HALO, ND, width), f32)

    dirs = lax.broadcasted_iota(jnp.int32, (ND, LANES), 0).astype(f32)
    heading = 2.0 * math.pi * (dirs + 0.5) / ND
    cos_h, sin_h = jnp.cos(heading), jnp.sin(heading)
    log_step = math.log(1.1)
    lats = [math.radians(-75.0 + 150.0 * (r + 0.5) / lat_count) for r in range(lat_count)]
    sea = [aux_ref[0:1, r * NLON : (r + 1) * NLON] for r in range(lat_count)]
    quarter = ND // 4
    tiles = NLON // LANES
    moments = [[jnp.zeros((quarter, NLON), f32) for _ in range(lat_count)] for _ in range(2)]
    for f in range(freq_dev):
        loads[f].wait()
        freq = (me * freq_dev + f).astype(f32)
        speed = 0.2 * jnp.exp(jnp.full((quarter, LANES), -log_step, f32) * freq)
        omega = jnp.exp(jnp.full((quarter, LANES), log_step, f32) * (freq - NF // 2))
        omega = jnp.concatenate([omega] * tiles, axis=1)
        sums = [None] * lat_count
        for q in range(4):
            east, north = q in (0, 3), q in (0, 1)
            rows = slice(f * ND + q * quarter, f * ND + (q + 1) * quarter)
            part = slice(q * quarter, (q + 1) * quarter)
            cx0 = speed * jnp.abs(cos_h[part])
            cy = jnp.concatenate([speed * jnp.abs(sin_h[part])] * tiles, axis=1)
            cx = [jnp.concatenate([cx0 * (1.0 / math.cos(a))] * tiles, axis=1) for a in lats]
            energy = [raw[rows, r * NLON : (r + 1) * NLON] * sea[r] for r in range(lat_count)]
            for _ in range(ADV_STEPS):
                fresh = []
                for r in range(lat_count):
                    e = energy[r]
                    side_x = pltpu.roll(e, 1 if east else NLON - 1, 1)
                    other = r - 1 if north else r + 1
                    side_y = energy[other] if 0 <= other < lat_count else 0.0
                    fresh.append((e - cx[r] * (e - side_x) - cy * (e - side_y)) * sea[r])
                energy = fresh
            for r in range(lat_count):
                adv[rows, r * NLON : (r + 1) * NLON] = energy[r]
                sums[r] = energy[r] if q == 0 else sums[r] + energy[r]
        for r in range(lat_count):
            moments[0][r] = moments[0][r] + sums[r]
            moments[1][r] = moments[1][r] + omega * sums[r]
    for i in range(2):
        for r in range(lat_count):
            mom_out[i : i + 1, r * NLON : (r + 1) * NLON] = jnp.sum(
                moments[i][r], axis=0, keepdims=True
            )

    pl.semaphore_wait(barrier, count - 1)

    def cells_of(index):
        return pl.ds(pl.multiple_of(index * width, LANES), width)

    for step in range(1, count):
        target = (me + step) % count
        remote(
            mom_out.at[:, cells_of(target % group)], mom_in.at[me],
            mom_send.at[step - 1], mom_recv.at[me], target,
        ).start()

    offsets = [(dy, dc) for dy in range(sides) for dc in range(2)]

    def rank_of(offset):
        return (side + offset[0]) % sides * 2 + (core + offset[1]) % 2

    def y_copy(f, i):
        peer = rank_of(offsets[i])
        return remote(
            adv.at[pl.ds(f * ND, ND), cells_of(peer)], held.at[HALO + rank * freq_dev + f],
            y_sem.at[i - 1, f], held_sem.at[HALO + rank * freq_dev + f], zone * group + peer,
        )

    def own_copy(f):
        slot = HALO + rank * freq_dev + f
        return pltpu.make_async_copy(
            adv.at[pl.ds(f * ND, ND), cells_of(rank)], held.at[slot], held_sem.at[slot]
        )

    for f in range(freq_dev):
        for i in list(range(2, group)) + [1]:
            y_copy(f, i).start()
        own_copy(f).start()
    local_mom = pltpu.make_async_copy(
        mom_out.at[:, cells_of(rank)], mom_in.at[me], mom_recv.at[me]
    )
    local_mom.start()

    wind[...] = (
        jnp.concatenate([cos_h] * (width // LANES), axis=1) * aux_ref[1:2, cells_of(rank)]
        + jnp.concatenate([sin_h] * (width // LANES), axis=1) * aux_ref[2:3, cells_of(rank)]
    )

    def up_copy(slot):
        return remote(
            held.at[HALO + slot], held.at[HALO + slot - freq_group],
            up_sem.at[slot - (freq_group - HALO)], held_sem.at[HALO + slot - freq_group],
            (zone + 1) % zones * group + rank,
        )

    def down_copy(slot):
        return remote(
            held.at[HALO + slot], held.at[HALO + slot + freq_group],
            down_sem.at[slot], held_sem.at[HALO + slot + freq_group],
            (zone + zones - 1) % zones * group + rank,
        )

    def arrive(index):
        remote(
            held.at[index], held.at[index], up_sem.at[0], held_sem.at[index],
            (me + 1) % count,
        ).wait_recv()

    for dy in range(sides):
        for f in range(freq_dev):
            for dc in range(2):
                slot = rank_of((dy, dc)) * freq_dev + f
                if (dy, dc) == (0, 0):
                    own_copy(f).wait()
                else:
                    arrive(HALO + slot)

                @pl.when((slot >= freq_group - HALO) & (zone < zones - 1))
                def _():
                    up_copy(slot).start()

                @pl.when((slot < HALO) & (zone > 0))
                def _():
                    down_copy(slot).start()

    local_mom.wait()
    for step in range(1, count):
        source = (me + step) % count
        remote(
            mom_in.at[source], mom_in.at[source], mom_send.at[0], mom_recv.at[source], source
        ).wait_recv()
    total = jnp.sum(mom_in[...], axis=0) * (1.0 / (NF * ND))
    energy_mean, moment_one = total[0:1], total[1:2]
    mean_freq = moment_one / (energy_mean + 1e-06)
    steepness = energy_mean * mean_freq * mean_freq
    breaking = steepness * steepness / (1.0 + steepness * steepness)

    acc[...] = jnp.zeros_like(acc)
    ascending = side > 0

    for i in range(HALO):
        early = jnp.where(ascending, i, HALO + freq_group + i)

        @pl.when(jnp.where(ascending, zone > 0, zone < zones - 1))
        def _():
            arrive(early)

    def ret_copy(k):
        owner, f = k // freq_dev, k % freq_dev
        return remote(
            done.at[k],
            out_ref.at[pl.ds(pl.multiple_of(f * ND, ND), ND), cells_of(rank)],
            ret_send.at[k], ret_recv.at[rank, f], zone * group + owner,
        )

    def ret_local(k):
        f = k % freq_dev
        return pltpu.make_async_copy(
            done.at[k],
            out_ref.at[pl.ds(pl.multiple_of(f * ND, ND), ND), cells_of(rank)],
            ret_recv.at[rank, f],
        )

    def source_step(i, carry):
        k = jnp.where(ascending, i, freq_group - 1 - i)
        late = i - (freq_group - HALO)

        @pl.when((late >= 0) & jnp.where(ascending, zone < zones - 1, zone > 0))
        def _():
            arrive(jnp.where(ascending, HALO + freq_group + late, HALO - 1 - late))

        freq = zone * freq_group + k

        def scale(index, factor):
            return jnp.where((index >= 3) & (index <= NF - 3), factor, 0.0).astype(f32)

        w_own, w_low, w_high = scale(freq, -0.002), scale(freq - 2, 0.001), scale(freq + 3, 0.001)
        omega = jnp.exp(
            jnp.full((1, LANES), log_step, f32) * (freq.astype(f32) - NF // 2)
        )
        for t in range(width // LANES):
            lanes = slice(t * LANES, (t + 1) * LANES)

            def slab(shift):
                return held[HALO + k + shift, :, lanes]

            def turn(values, amount):
                return pltpu.roll(values, amount % ND, 0)

            def rate(a, p, m):
                return a * (a * (p + m) - 2.0 * (p * m))

            own = slab(0)
            p2, m3, m2, m5, p3, p5 = (slab(s) for s in (2, -3, -2, -5, 3, 5))
            near = rate(own, turn(p2, -1), turn(m3, 3)) + rate(own, turn(p2, 1), turn(m3, -3))
            low = rate(turn(m2, 1), own, turn(m5, 4)) + rate(turn(m2, -1), own, turn(m5, -4))
            high = rate(turn(p3, -3), turn(p5, -4), own) + rate(turn(p3, 3), turn(p5, 4), own)
            interaction = w_own * near + w_low * low + w_high * high
            gain = (0.05 * omega) * jnp.maximum(0.0, wind[:, lanes] * omega - 1.0)
            damping = (0.03 * omega) * breaking[:, lanes]
            fresh = own + (gain - damping) * own + interaction
            done[k, :, lanes] = fresh
            acc[:, lanes] += fresh

        @pl.when(k // freq_dev == rank)
        def _():
            ret_local(k).start()

        @pl.when(k // freq_dev != rank)
        def _():
            ret_copy(k).start()

        return carry

    lax.fori_loop(0, freq_group, source_step, 0)

    sum_out[...] = jnp.sum(acc[...], axis=0, keepdims=True)

    def sum_copy(step):
        return remote(
            sum_out, sum_in.at[me], sum_send.at[step - 1], sum_recv.at[me], (me + step) % count
        )

    for step in range(1, count):
        sum_copy(step).start()
    sum_in[me] = sum_out[...]
    for step in range(1, count):
        source = (me + step) % count
        remote(
            sum_out, sum_in.at[source], sum_send.at[0], sum_recv.at[source], source
        ).wait_recv()

    per_row = count // group
    mine_row = me // per_row
    height_sum = jnp.zeros((1, width), f32)
    mine = jnp.zeros((1, width), f32)
    for g in range(group):
        mass = sum_in[g]
        for other in range(1, zones):
            mass = mass + sum_in[other * group + g]
        sea_row = aux_ref[0:1, g * width : (g + 1) * width]
        height = sea_row * (4.0 * jnp.sqrt(mass * (1.0 / (NF * ND)) + 1e-06))
        height_sum = height_sum + height
        mine = jnp.where(mine_row == g, height, mine)
    points = cells // count
    shift = (me % per_row) * points
    turned = pltpu.roll(jnp.broadcast_to(mine, (8, width)), (width - shift) % width, 1)
    wave_ref[...] = turned[0:1, :points]
    mean_ref[...] = jnp.sum(height_sum, axis=1, keepdims=True) * (1.0 / (SEA_DEV * count))

    for f in range(freq_dev):
        for i in range(1, group):
            peer = rank_of(offsets[i])
            remote(
                done.at[0], out_ref.at[pl.ds(f * ND, ND), cells_of(peer)],
                ret_send.at[0], ret_recv.at[peer, f], zone * group + peer,
            ).wait_recv()
            y_copy(f, i).wait_send()
            ret_copy(peer * freq_dev + f).wait_send()
        ret_local(rank * freq_dev + f).wait()
    for step in range(1, count):
        remote(
            mom_out.at[:, cells_of(0)], mom_in.at[me], mom_send.at[step - 1],
            mom_recv.at[me], (me + step) % count,
        ).wait_send()
        sum_copy(step).wait_send()

    @pl.when(zone < zones - 1)
    def _():
        for slot in range(freq_group - HALO, freq_group):
            up_copy(slot).wait_send()

    @pl.when(zone > 0)
    def _():
        for slot in range(HALO):
            down_copy(slot).wait_send()


def fused_local(spectrum, sea_mask, wind_speed, wind_angle):
    count = lax.axis_size("spec")
    bins_dev, cells = spectrum.shape
    group = group_size(count, bins_dev, cells)
    freq_dev = bins_dev // ND
    freq_group = freq_dev * group
    width = cells // group
    points = cells // count
    aux = jnp.stack(
        [
            sea_mask.astype(jnp.float32),
            wind_speed * jnp.cos(wind_angle),
            wind_speed * jnp.sin(wind_angle),
        ]
    )
    f32 = jnp.float32
    dma = pltpu.SemaphoreType.DMA
    out, wave, mean = pl.pallas_call(
        functools.partial(fused_kernel, count, group),
        out_shape=(
            jax.ShapeDtypeStruct((bins_dev, cells), f32),
            jax.ShapeDtypeStruct((1, points), f32),
            jax.ShapeDtypeStruct((1, 1), f32),
        ),
        in_specs=[
            pl.BlockSpec(memory_space=pltpu.VMEM),
            pl.BlockSpec(memory_space=pl.ANY),
        ],
        out_specs=(
            pl.BlockSpec(memory_space=pl.ANY),
            pl.BlockSpec(memory_space=pltpu.VMEM),
            pl.BlockSpec(memory_space=pltpu.VMEM),
        ),
        scratch_shapes=[
            pltpu.VMEM((bins_dev, cells), f32),
            pltpu.VMEM((bins_dev, cells), f32),
            pltpu.VMEM((freq_group + 2 * HALO, ND, width), f32),
            pltpu.VMEM((freq_group, ND, width), f32),
            pltpu.VMEM((2, cells), f32),
            pltpu.VMEM((count, 2, width), f32),
            pltpu.VMEM((ND, width), f32),
            pltpu.VMEM((ND, width), f32),
            pltpu.VMEM((1, width), f32),
            pltpu.VMEM((count, 1, width), f32),
            dma((freq_dev,)),
            dma((freq_group + 2 * HALO,)),
            dma((group - 1, freq_dev)),
            dma((HALO,)),
            dma((HALO,)),
            dma((count - 1,)),
            dma((count,)),
            dma((freq_group,)),
            dma((group, freq_dev)),
            dma((count - 1,)),
            dma((count,)),
        ],
        compiler_params=pltpu.CompilerParams(collective_id=0, has_side_effects=True),
    )(aux, spectrum)
    return (out, wave.reshape(points), mean.reshape(1))


def solution(mesh):
    in_specs = (P(("grp", "spec"), None), P(), P("grp"), P("grp"))
    out_specs = (P(("grp", "spec"), None), P(("grp", "spec")), P("grp"))

    def body(spectrum, sea_mask, wind_speed, wind_angle):
        fits = group_size(mesh.shape["spec"], *spectrum.shape)
        plan = fused_local if fits else local
        return plan(spectrum, sea_mask, wind_speed, wind_angle)

    return jax.shard_map(body, mesh=mesh, in_specs=in_specs, out_specs=out_specs, check_vma=False)
```

```python
import functools
import math

import jax
import jax.numpy as jnp
from jax import lax
from jax.experimental import pallas as pl
from jax.experimental.pallas import tpu as pltpu
from jax.sharding import PartitionSpec as P

NF = 48
ND = 32
NLON = 384
ADV_STEPS = 2
SEA_DEV = 64


def upwind_step(energy, courant_x, courant_y, sea_grid):
    west_cell = jnp.roll(energy, 1, axis=2)
    east_cell = jnp.roll(energy, -1, axis=2)
    edge_row = jnp.zeros_like(energy[:, :1])
    south_cell = jnp.concatenate([edge_row, energy[:, :-1]], axis=1)
    north_cell = jnp.concatenate([energy[:, 1:], edge_row], axis=1)
    updated = (
        energy
        - jnp.maximum(courant_x, 0.0) * (energy - west_cell)
        - jnp.minimum(courant_x, 0.0) * (east_cell - energy)
        - jnp.maximum(courant_y, 0.0) * (energy - south_cell)
        - jnp.minimum(courant_y, 0.0) * (north_cell - energy)
    )
    return updated * sea_grid


def courant_numbers(freq_index, dir_index, lat_count, dir_count):
    speed = 0.2 * jnp.exp(-math.log(1.1) * freq_index)
    heading = 2.0 * math.pi * (dir_index + 0.5) / dir_count
    rows = jnp.arange(lat_count, dtype=jnp.float32)
    latitude = (-75.0 + 150.0 * (rows + 0.5) / lat_count) * (math.pi / 180.0)
    courant_x = (speed * jnp.cos(heading))[:, None, None] / jnp.cos(latitude)[None, :, None]
    courant_y = (speed * jnp.sin(heading))[:, None, None]
    return (courant_x, courant_y)


def shift_freq(values, amount):
    if amount > 0:
        filler = jnp.zeros_like(values[:amount])
        return jnp.concatenate([filler, values[:-amount]], axis=0)
    filler = jnp.zeros_like(values[:-amount])
    return jnp.concatenate([values[-amount:], filler], axis=0)


def source_terms(energy, speed, angle):
    freq_count = energy.shape[0]
    dir_count = energy.shape[1]
    freq_ids = jnp.arange(freq_count, dtype=jnp.float32)
    frequency = jnp.exp(math.log(1.1) * (freq_ids - freq_count // 2))[:, None, None]
    heading = (2.0 * math.pi * (jnp.arange(dir_count, dtype=jnp.float32) + 0.5) / dir_count)[
        None, :, None
    ]
    energy_mean = jnp.mean(energy, axis=(0, 1))
    moment_one = jnp.mean(frequency * energy, axis=(0, 1))
    mean_freq = moment_one / (energy_mean + 1e-06)
    steepness = energy_mean * mean_freq * mean_freq
    breaking = steepness * steepness / (1.0 + steepness * steepness)
    wind_gain = (
        0.05
        * frequency
        * jnp.maximum(
            0.0, speed[None, None, :] * frequency * jnp.cos(heading - angle[None, None, :]) - 1.0
        )
    )
    damping = 0.03 * frequency * breaking[None, None, :]
    valid = ((freq_ids >= 3) & (freq_ids <= freq_count - 3)).astype(jnp.float32)[:, None, None]
    interaction = jnp.zeros_like(energy)
    for mirror in (1, -1):
        plus_bins = shift_freq(jnp.roll(energy, -mirror, axis=1), -2)
        minus_bins = shift_freq(jnp.roll(energy, 3 * mirror, axis=1), 3)
        transfer_rate = (
            0.001
            * valid
            * (energy * energy * (plus_bins + minus_bins) - 2.0 * energy * plus_bins * minus_bins)
        )
        interaction = interaction - 2.0 * transfer_rate
        interaction = interaction + jnp.roll(shift_freq(transfer_rate, 2), mirror, axis=1)
        interaction = interaction + jnp.roll(shift_freq(transfer_rate, -3), -3 * mirror, axis=1)
    updated = energy + (wind_gain - damping) * energy + interaction
    raw_height = 4.0 * jnp.sqrt(jnp.mean(updated, axis=(0, 1)) + 1e-06)
    return (updated, raw_height)


def local(spectrum, sea_mask, wind_speed, wind_angle):
    count = lax.axis_size("spec")
    position = lax.axis_index("spec")
    bins_dev = spectrum.shape[0]
    cells = spectrum.shape[1]
    points = cells // count
    lat_count = cells // NLON
    sea_float = sea_mask.astype(jnp.float32)
    bin_ids = position * bins_dev + jnp.arange(bins_dev, dtype=jnp.int32)
    freq_index = (bin_ids // ND).astype(jnp.float32)
    dir_index = (bin_ids % ND).astype(jnp.float32)
    courant_x, courant_y = courant_numbers(freq_index, dir_index, lat_count, ND)
    sea_grid = sea_float.reshape(1, lat_count, NLON)
    energy = (spectrum * sea_float[None, :]).reshape(bins_dev, lat_count, NLON)
    for substep in range(ADV_STEPS):
        energy = upwind_step(energy, courant_x, courant_y, sea_grid)
    advected = energy.reshape(bins_dev, cells)
    outgoing = advected.reshape(bins_dev, count, points)
    arrived = lax.all_to_all(outgoing, "spec", split_axis=1, concat_axis=0, tiled=True)
    start = position * points
    speed_own = lax.dynamic_slice_in_dim(wind_speed, start, points)
    angle_own = lax.dynamic_slice_in_dim(wind_angle, start, points)
    sea_own = lax.dynamic_slice_in_dim(sea_float, start, points)
    updated, raw_height = source_terms(arrived.reshape(NF, ND, points), speed_own, angle_own)
    wave_height = sea_own * raw_height
    own_total = jnp.zeros((count, 1), jnp.float32) + jnp.sum(wave_height)
    returned, totals = (
        lax.all_to_all(
            updated.reshape(NF * ND, 1, points), "spec", split_axis=0, concat_axis=1, tiled=True
        ),
        lax.all_to_all(own_total, "spec", split_axis=0, concat_axis=1, tiled=True),
    )
    new_spectrum = returned.reshape(bins_dev, cells)
    height_sum = jnp.sum(totals)
    mean_height = (height_sum / (SEA_DEV * count)).reshape(1)
    return (new_spectrum, wave_height, mean_height)


HALO = 5
LANES = 128


def group_size(count, bins_dev, cells):
    size = 4
    if count % size or bins_dev % ND or cells % (size * LANES) or cells % NLON:
        return 0
    if NLON % LANES or bins_dev // ND * size < 2 * HALO or cells % count:
        return 0
    return size


def fused_kernel(
    count, group, sea_in, wind_in, angle_in, spec_ref, out_ref, wave_ref, mean_ref,
    sea_raw, wind_raw, aux_ref, aux_sem,
    raw, adv, held, done, mom_out, mom_in, wind, acc, sum_out, sum_in,
    load_sem, held_sem, y_sem, up_sem, down_sem, mom_send, mom_recv,
    ret_send, ret_recv, sum_send, sum_recv,
):
    f32 = jnp.float32
    bins_dev, cells = adv.shape
    freq_dev = bins_dev // ND
    freq_group = freq_dev * group
    width = cells // group
    zones = count // group
    lat_count = cells // NLON
    sides = group // 2
    me = lax.axis_index("spec")
    zone, rank = me // group, me % group
    side, core = rank // 2, rank % 2

    def remote(src, dst, send, recv, target):
        return pltpu.make_async_remote_copy(
            src_ref=src, dst_ref=dst, send_sem=send, recv_sem=recv,
            device_id={"spec": target}, device_id_type=pl.DeviceIdType.MESH,
        )

    barrier = pltpu.get_barrier_semaphore()
    for step in range(1, count):
        pl.semaphore_signal(
            barrier, inc=1, device_id={"spec": (me + step) % count},
            device_id_type=pl.DeviceIdType.MESH,
        )
    loads = [
        pltpu.make_async_copy(
            spec_ref.at[pl.ds(f * ND, ND)], raw.at[pl.ds(f * ND, ND)], load_sem.at[f]
        )
        for f in range(freq_dev)
    ]
    small = [
        pltpu.make_async_copy(sea_in, sea_raw, aux_sem.at[0]),
        pltpu.make_async_copy(wind_in, wind_raw.at[0:1], aux_sem.at[1]),
        pltpu.make_async_copy(angle_in, wind_raw.at[1:2], aux_sem.at[2]),
    ]
    for load in small[:1] + loads + small[1:]:
        load.start()

    @pl.when(zone == 0)
    def _():
        held[0:HALO] = jnp.zeros((HALO, ND, width), f32)

    @pl.when(zone == zones - 1)
    def _():
        held[HALO + freq_group :] = jnp.zeros((HALO, ND, width), f32)

    dirs = lax.broadcasted_iota(jnp.int32, (ND, LANES), 0).astype(f32)
    heading = 2.0 * math.pi * (dirs + 0.5) / ND
    cos_h, sin_h = jnp.cos(heading), jnp.sin(heading)
    log_step = math.log(1.1)
    lats = [math.radians(-75.0 + 150.0 * (r + 0.5) / lat_count) for r in range(lat_count)]
    small[0].wait()
    aux_ref[0:1] = sea_raw[...].astype(f32)
    sea = [aux_ref[0:1, r * NLON : (r + 1) * NLON] for r in range(lat_count)]
    quarter = ND // 4
    tiles = NLON // LANES
    moments = [[jnp.zeros((quarter, NLON), f32) for _ in range(lat_count)] for _ in range(2)]
    for f in range(freq_dev):
        loads[f].wait()
        freq = (me * freq_dev + f).astype(f32)
        speed = 0.2 * jnp.exp(jnp.full((quarter, LANES), -log_step, f32) * freq)
        omega = jnp.exp(jnp.full((quarter, LANES), log_step, f32) * (freq - NF // 2))
        omega = jnp.concatenate([omega] * tiles, axis=1)
        sums = [None] * lat_count
        for q in range(4):
            east, north = q in (0, 3), q in (0, 1)
            rows = slice(f * ND + q * quarter, f * ND + (q + 1) * quarter)
            part = slice(q * quarter, (q + 1) * quarter)
            cx0 = speed * jnp.abs(cos_h[part])
            cy = jnp.concatenate([speed * jnp.abs(sin_h[part])] * tiles, axis=1)
            cx = [jnp.concatenate([cx0 * (1.0 / math.cos(a))] * tiles, axis=1) for a in lats]
            energy = [raw[rows, r * NLON : (r + 1) * NLON] * sea[r] for r in range(lat_count)]
            for _ in range(ADV_STEPS):
                fresh = []
                for r in range(lat_count):
                    e = energy[r]
                    side_x = pltpu.roll(e, 1 if east else NLON - 1, 1)
                    other = r - 1 if north else r + 1
                    side_y = energy[other] if 0 <= other < lat_count else 0.0
                    fresh.append((e - cx[r] * (e - side_x) - cy * (e - side_y)) * sea[r])
                energy = fresh
            for r in range(lat_count):
                adv[rows, r * NLON : (r + 1) * NLON] = energy[r]
                sums[r] = energy[r] if q == 0 else sums[r] + energy[r]
        for r in range(lat_count):
            moments[0][r] = moments[0][r] + sums[r]
            moments[1][r] = moments[1][r] + omega * sums[r]
    for i in range(2):
        for r in range(lat_count):
            mom_out[i : i + 1, r * NLON : (r + 1) * NLON] = jnp.sum(
                moments[i][r], axis=0, keepdims=True
            )

    pl.semaphore_wait(barrier, count - 1)

    def cells_of(index):
        return pl.ds(pl.multiple_of(index * width, LANES), width)

    for step in range(1, count):
        target = (me + step) % count
        remote(
            mom_out.at[:, cells_of(target % group)], mom_in.at[me],
            mom_send.at[step - 1], mom_recv.at[me], target,
        ).start()

    offsets = [(dy, dc) for dy in range(sides) for dc in range(2)]

    def rank_of(offset):
        return (side + offset[0]) % sides * 2 + (core + offset[1]) % 2

    def y_copy(f, i):
        peer = rank_of(offsets[i])
        return remote(
            adv.at[pl.ds(f * ND, ND), cells_of(peer)], held.at[HALO + rank * freq_dev + f],
            y_sem.at[i - 1, f], held_sem.at[HALO + rank * freq_dev + f], zone * group + peer,
        )

    def own_copy(f):
        slot = HALO + rank * freq_dev + f
        return pltpu.make_async_copy(
            adv.at[pl.ds(f * ND, ND), cells_of(rank)], held.at[slot], held_sem.at[slot]
        )

    for f in range(freq_dev):
        for i in list(range(2, group)) + [1]:
            y_copy(f, i).start()
        own_copy(f).start()
    local_mom = pltpu.make_async_copy(
        mom_out.at[:, cells_of(rank)], mom_in.at[me], mom_recv.at[me]
    )
    local_mom.start()

    small[1].wait()
    small[2].wait()
    speed_own, angle_own = wind_raw[0:1, cells_of(rank)], wind_raw[1:2, cells_of(rank)]
    wind[...] = jnp.concatenate([cos_h] * (width // LANES), axis=1) * (
        speed_own * jnp.cos(angle_own)
    ) + jnp.concatenate([sin_h] * (width // LANES), axis=1) * (speed_own * jnp.sin(angle_own))

    def up_copy(slot):
        return remote(
            held.at[HALO + slot], held.at[HALO + slot - freq_group],
            up_sem.at[slot - (freq_group - HALO)], held_sem.at[HALO + slot - freq_group],
            (zone + 1) % zones * group + rank,
        )

    def down_copy(slot):
        return remote(
            held.at[HALO + slot], held.at[HALO + slot + freq_group],
            down_sem.at[slot], held_sem.at[HALO + slot + freq_group],
            (zone + zones - 1) % zones * group + rank,
        )

    def arrive(index):
        remote(
            held.at[index], held.at[index], up_sem.at[0], held_sem.at[index],
            (me + 1) % count,
        ).wait_recv()

    for dy in range(sides):
        for f in range(freq_dev):
            for dc in range(2):
                slot = rank_of((dy, dc)) * freq_dev + f
                if (dy, dc) == (0, 0):
                    own_copy(f).wait()
                else:
                    arrive(HALO + slot)

                @pl.when((slot >= freq_group - HALO) & (zone < zones - 1))
                def _():
                    up_copy(slot).start()

                @pl.when((slot < HALO) & (zone > 0))
                def _():
                    down_copy(slot).start()

    local_mom.wait()
    for step in range(1, count):
        source = (me + step) % count
        remote(
            mom_in.at[source], mom_in.at[source], mom_send.at[0], mom_recv.at[source], source
        ).wait_recv()
    total = jnp.sum(mom_in[...], axis=0) * (1.0 / (NF * ND))
    energy_mean, moment_one = total[0:1], total[1:2]
    mean_freq = moment_one / (energy_mean + 1e-06)
    steepness = energy_mean * mean_freq * mean_freq
    breaking = steepness * steepness / (1.0 + steepness * steepness)

    acc[...] = jnp.zeros_like(acc)
    ascending = side > 0

    for i in range(HALO):
        early = jnp.where(ascending, i, HALO + freq_group + i)

        @pl.when(jnp.where(ascending, zone > 0, zone < zones - 1))
        def _():
            arrive(early)

    def ret_copy(k):
        owner, f = k // freq_dev, k % freq_dev
        return remote(
            done.at[k],
            out_ref.at[pl.ds(pl.multiple_of(f * ND, ND), ND), cells_of(rank)],
            ret_send.at[k], ret_recv.at[rank, f], zone * group + owner,
        )

    def ret_local(k):
        f = k % freq_dev
        return pltpu.make_async_copy(
            done.at[k],
            out_ref.at[pl.ds(pl.multiple_of(f * ND, ND), ND), cells_of(rank)],
            ret_recv.at[rank, f],
        )

    def source_step(i, carry):
        k = jnp.where(ascending, i, freq_group - 1 - i)
        late = i - (freq_group - HALO)

        @pl.when((late >= 0) & jnp.where(ascending, zone < zones - 1, zone > 0))
        def _():
            arrive(jnp.where(ascending, HALO + freq_group + late, HALO - 1 - late))

        freq = zone * freq_group + k

        def scale(index, factor):
            return jnp.where((index >= 3) & (index <= NF - 3), factor, 0.0).astype(f32)

        w_own, w_low, w_high = scale(freq, -0.002), scale(freq - 2, 0.001), scale(freq + 3, 0.001)
        omega = jnp.exp(
            jnp.full((1, LANES), log_step, f32) * (freq.astype(f32) - NF // 2)
        )
        for t in range(width // LANES):
            lanes = slice(t * LANES, (t + 1) * LANES)

            def slab(shift):
                return held[HALO + k + shift, :, lanes]

            def turn(values, amount):
                return pltpu.roll(values, amount % ND, 0)

            def rate(a, p, m):
                return a * (a * (p + m) - 2.0 * (p * m))

            own = slab(0)
            p2, m3, m2, m5, p3, p5 = (slab(s) for s in (2, -3, -2, -5, 3, 5))
            near = rate(own, turn(p2, -1), turn(m3, 3)) + rate(own, turn(p2, 1), turn(m3, -3))
            low = rate(turn(m2, 1), own, turn(m5, 4)) + rate(turn(m2, -1), own, turn(m5, -4))
            high = rate(turn(p3, -3), turn(p5, -4), own) + rate(turn(p3, 3), turn(p5, 4), own)
            interaction = w_own * near + w_low * low + w_high * high
            gain = (0.05 * omega) * jnp.maximum(0.0, wind[:, lanes] * omega - 1.0)
            damping = (0.03 * omega) * breaking[:, lanes]
            fresh = own + (gain - damping) * own + interaction
            done[k, :, lanes] = fresh
            acc[:, lanes] += fresh

        @pl.when(k // freq_dev == rank)
        def _():
            ret_local(k).start()

        @pl.when(k // freq_dev != rank)
        def _():
            ret_copy(k).start()

        return carry

    lax.fori_loop(0, freq_group, source_step, 0)

    sum_out[...] = jnp.sum(acc[...], axis=0, keepdims=True)

    def sum_copy(step):
        return remote(
            sum_out, sum_in.at[me], sum_send.at[step - 1], sum_recv.at[me], (me + step) % count
        )

    for step in range(1, count):
        sum_copy(step).start()
    sum_in[me] = sum_out[...]
    for step in range(1, count):
        source = (me + step) % count
        remote(
            sum_out, sum_in.at[source], sum_send.at[0], sum_recv.at[source], source
        ).wait_recv()

    per_row = count // group
    mine_row = me // per_row
    height_sum = jnp.zeros((1, width), f32)
    mine = jnp.zeros((1, width), f32)
    for g in range(group):
        mass = sum_in[g]
        for other in range(1, zones):
            mass = mass + sum_in[other * group + g]
        sea_row = aux_ref[0:1, g * width : (g + 1) * width]
        height = sea_row * (4.0 * jnp.sqrt(mass * (1.0 / (NF * ND)) + 1e-06))
        height_sum = height_sum + height
        mine = jnp.where(mine_row == g, height, mine)
    points = cells // count
    shift = (me % per_row) * points
    turned = pltpu.roll(jnp.broadcast_to(mine, (8, width)), (width - shift) % width, 1)
    wave_ref[...] = turned[0:1, :points]
    mean_ref[...] = jnp.sum(height_sum, axis=1, keepdims=True) * (1.0 / (SEA_DEV * count))

    for f in range(freq_dev):
        for i in range(1, group):
            peer = rank_of(offsets[i])
            remote(
                done.at[0], out_ref.at[pl.ds(f * ND, ND), cells_of(peer)],
                ret_send.at[0], ret_recv.at[peer, f], zone * group + peer,
            ).wait_recv()
            y_copy(f, i).wait_send()
            ret_copy(peer * freq_dev + f).wait_send()
        ret_local(rank * freq_dev + f).wait()
    for step in range(1, count):
        remote(
            mom_out.at[:, cells_of(0)], mom_in.at[me], mom_send.at[step - 1],
            mom_recv.at[me], (me + step) % count,
        ).wait_send()
        sum_copy(step).wait_send()

    @pl.when(zone < zones - 1)
    def _():
        for slot in range(freq_group - HALO, freq_group):
            up_copy(slot).wait_send()

    @pl.when(zone > 0)
    def _():
        for slot in range(HALO):
            down_copy(slot).wait_send()


def fused_local(spectrum, sea_mask, wind_speed, wind_angle):
    count = lax.axis_size("spec")
    bins_dev, cells = spectrum.shape
    group = group_size(count, bins_dev, cells)
    freq_dev = bins_dev // ND
    freq_group = freq_dev * group
    width = cells // group
    points = cells // count
    f32 = jnp.float32
    dma = pltpu.SemaphoreType.DMA
    out, wave, mean = pl.pallas_call(
        functools.partial(fused_kernel, count, group),
        out_shape=(
            pltpu.VMEM((bins_dev, cells), f32),
            jax.ShapeDtypeStruct((1, points), f32),
            jax.ShapeDtypeStruct((1, 1), f32),
        ),
        in_specs=[
            pl.BlockSpec(memory_space=pl.ANY),
        ]
        * 4,
        out_specs=(
            pl.BlockSpec(memory_space=pltpu.VMEM),
            pl.BlockSpec(memory_space=pltpu.VMEM),
            pl.BlockSpec(memory_space=pltpu.VMEM),
        ),
        scratch_shapes=[
            pltpu.VMEM((1, cells), jnp.int32),
            pltpu.VMEM((2, cells), f32),
            pltpu.VMEM((1, cells), f32),
            dma((3,)),
            pltpu.VMEM((bins_dev, cells), f32),
            pltpu.VMEM((bins_dev, cells), f32),
            pltpu.VMEM((freq_group + 2 * HALO, ND, width), f32),
            pltpu.VMEM((freq_group, ND, width), f32),
            pltpu.VMEM((2, cells), f32),
            pltpu.VMEM((count, 2, width), f32),
            pltpu.VMEM((ND, width), f32),
            pltpu.VMEM((ND, width), f32),
            pltpu.VMEM((1, width), f32),
            pltpu.VMEM((count, 1, width), f32),
            dma((freq_dev,)),
            dma((freq_group + 2 * HALO,)),
            dma((group - 1, freq_dev)),
            dma((HALO,)),
            dma((HALO,)),
            dma((count - 1,)),
            dma((count,)),
            dma((freq_group,)),
            dma((group, freq_dev)),
            dma((count - 1,)),
            dma((count,)),
        ],
        compiler_params=pltpu.CompilerParams(collective_id=0, has_side_effects=True),
    )(
        sea_mask.reshape(1, cells),
        wind_speed.reshape(1, cells),
        wind_angle.reshape(1, cells),
        spectrum,
    )
    return (out, wave.reshape(points), mean.reshape(1))


def solution(mesh):
    in_specs = (P(("grp", "spec"), None), P(), P("grp"), P("grp"))
    out_specs = (P(("grp", "spec"), None), P(("grp", "spec")), P("grp"))

    def body(spectrum, sea_mask, wind_speed, wind_angle):
        fits = group_size(mesh.shape["spec"], *spectrum.shape)
        plan = fused_local if fits else local
        return plan(spectrum, sea_mask, wind_speed, wind_angle)

    return jax.shard_map(body, mesh=mesh, in_specs=in_specs, out_specs=out_specs, check_vma=False)
```

```python
import functools
import math

import jax
import jax.numpy as jnp
from jax import lax
from jax.experimental import pallas as pl
from jax.experimental.pallas import tpu as pltpu
from jax.sharding import PartitionSpec as P

NF = 48
ND = 32
NLON = 384
ADV_STEPS = 2
SEA_DEV = 64


def upwind_step(energy, courant_x, courant_y, sea_grid):
    west_cell = jnp.roll(energy, 1, axis=2)
    east_cell = jnp.roll(energy, -1, axis=2)
    edge_row = jnp.zeros_like(energy[:, :1])
    south_cell = jnp.concatenate([edge_row, energy[:, :-1]], axis=1)
    north_cell = jnp.concatenate([energy[:, 1:], edge_row], axis=1)
    updated = (
        energy
        - jnp.maximum(courant_x, 0.0) * (energy - west_cell)
        - jnp.minimum(courant_x, 0.0) * (east_cell - energy)
        - jnp.maximum(courant_y, 0.0) * (energy - south_cell)
        - jnp.minimum(courant_y, 0.0) * (north_cell - energy)
    )
    return updated * sea_grid


def courant_numbers(freq_index, dir_index, lat_count, dir_count):
    speed = 0.2 * jnp.exp(-math.log(1.1) * freq_index)
    heading = 2.0 * math.pi * (dir_index + 0.5) / dir_count
    rows = jnp.arange(lat_count, dtype=jnp.float32)
    latitude = (-75.0 + 150.0 * (rows + 0.5) / lat_count) * (math.pi / 180.0)
    courant_x = (speed * jnp.cos(heading))[:, None, None] / jnp.cos(latitude)[None, :, None]
    courant_y = (speed * jnp.sin(heading))[:, None, None]
    return (courant_x, courant_y)


def shift_freq(values, amount):
    if amount > 0:
        filler = jnp.zeros_like(values[:amount])
        return jnp.concatenate([filler, values[:-amount]], axis=0)
    filler = jnp.zeros_like(values[:-amount])
    return jnp.concatenate([values[-amount:], filler], axis=0)


def source_terms(energy, speed, angle):
    freq_count = energy.shape[0]
    dir_count = energy.shape[1]
    freq_ids = jnp.arange(freq_count, dtype=jnp.float32)
    frequency = jnp.exp(math.log(1.1) * (freq_ids - freq_count // 2))[:, None, None]
    heading = (2.0 * math.pi * (jnp.arange(dir_count, dtype=jnp.float32) + 0.5) / dir_count)[
        None, :, None
    ]
    energy_mean = jnp.mean(energy, axis=(0, 1))
    moment_one = jnp.mean(frequency * energy, axis=(0, 1))
    mean_freq = moment_one / (energy_mean + 1e-06)
    steepness = energy_mean * mean_freq * mean_freq
    breaking = steepness * steepness / (1.0 + steepness * steepness)
    wind_gain = (
        0.05
        * frequency
        * jnp.maximum(
            0.0, speed[None, None, :] * frequency * jnp.cos(heading - angle[None, None, :]) - 1.0
        )
    )
    damping = 0.03 * frequency * breaking[None, None, :]
    valid = ((freq_ids >= 3) & (freq_ids <= freq_count - 3)).astype(jnp.float32)[:, None, None]
    interaction = jnp.zeros_like(energy)
    for mirror in (1, -1):
        plus_bins = shift_freq(jnp.roll(energy, -mirror, axis=1), -2)
        minus_bins = shift_freq(jnp.roll(energy, 3 * mirror, axis=1), 3)
        transfer_rate = (
            0.001
            * valid
            * (energy * energy * (plus_bins + minus_bins) - 2.0 * energy * plus_bins * minus_bins)
        )
        interaction = interaction - 2.0 * transfer_rate
        interaction = interaction + jnp.roll(shift_freq(transfer_rate, 2), mirror, axis=1)
        interaction = interaction + jnp.roll(shift_freq(transfer_rate, -3), -3 * mirror, axis=1)
    updated = energy + (wind_gain - damping) * energy + interaction
    raw_height = 4.0 * jnp.sqrt(jnp.mean(updated, axis=(0, 1)) + 1e-06)
    return (updated, raw_height)


def local(spectrum, sea_mask, wind_speed, wind_angle):
    count = lax.axis_size("spec")
    position = lax.axis_index("spec")
    bins_dev = spectrum.shape[0]
    cells = spectrum.shape[1]
    points = cells // count
    lat_count = cells // NLON
    sea_float = sea_mask.astype(jnp.float32)
    bin_ids = position * bins_dev + jnp.arange(bins_dev, dtype=jnp.int32)
    freq_index = (bin_ids // ND).astype(jnp.float32)
    dir_index = (bin_ids % ND).astype(jnp.float32)
    courant_x, courant_y = courant_numbers(freq_index, dir_index, lat_count, ND)
    sea_grid = sea_float.reshape(1, lat_count, NLON)
    energy = (spectrum * sea_float[None, :]).reshape(bins_dev, lat_count, NLON)
    for substep in range(ADV_STEPS):
        energy = upwind_step(energy, courant_x, courant_y, sea_grid)
    advected = energy.reshape(bins_dev, cells)
    outgoing = advected.reshape(bins_dev, count, points)
    arrived = lax.all_to_all(outgoing, "spec", split_axis=1, concat_axis=0, tiled=True)
    start = position * points
    speed_own = lax.dynamic_slice_in_dim(wind_speed, start, points)
    angle_own = lax.dynamic_slice_in_dim(wind_angle, start, points)
    sea_own = lax.dynamic_slice_in_dim(sea_float, start, points)
    updated, raw_height = source_terms(arrived.reshape(NF, ND, points), speed_own, angle_own)
    wave_height = sea_own * raw_height
    own_total = jnp.zeros((count, 1), jnp.float32) + jnp.sum(wave_height)
    returned, totals = (
        lax.all_to_all(
            updated.reshape(NF * ND, 1, points), "spec", split_axis=0, concat_axis=1, tiled=True
        ),
        lax.all_to_all(own_total, "spec", split_axis=0, concat_axis=1, tiled=True),
    )
    new_spectrum = returned.reshape(bins_dev, cells)
    height_sum = jnp.sum(totals)
    mean_height = (height_sum / (SEA_DEV * count)).reshape(1)
    return (new_spectrum, wave_height, mean_height)


HALO = 5
LANES = 128


def group_size(count, bins_dev, cells):
    size = 4
    if count % size or bins_dev % ND or cells % (size * LANES) or cells % NLON:
        return 0
    if NLON % LANES or bins_dev // ND * size < 2 * HALO or cells % count:
        return 0
    return size


def fused_kernel(
    count, group, sea_in, wind_in, angle_in, spec_ref, out_ref, wave_ref, mean_ref,
    sea_raw, wind_raw, angle_raw, aux_ref, aux_sem,
    raw, adv, held, done, mom_out, mom_in, wind, acc, sum_out, sum_in,
    load_sem, held_sem, y_sem, up_sem, down_sem, mom_send, mom_recv,
    ret_send, ret_recv, sum_send, sum_recv,
):
    f32 = jnp.float32
    bins_dev, cells = adv.shape
    freq_dev = bins_dev // ND
    freq_group = freq_dev * group
    width = cells // group
    zones = count // group
    lat_count = cells // NLON
    sides = group // 2
    me = lax.axis_index("spec")
    zone, rank = me // group, me % group
    side, core = rank // 2, rank % 2

    def remote(src, dst, send, recv, target):
        return pltpu.make_async_remote_copy(
            src_ref=src, dst_ref=dst, send_sem=send, recv_sem=recv,
            device_id={"spec": target}, device_id_type=pl.DeviceIdType.MESH,
        )

    barrier = pltpu.get_barrier_semaphore()
    for step in range(1, count):
        pl.semaphore_signal(
            barrier, inc=1, device_id={"spec": (me + step) % count},
            device_id_type=pl.DeviceIdType.MESH,
        )
    loads = [
        pltpu.make_async_copy(
            spec_ref.at[pl.ds(f * ND, ND)], raw.at[pl.ds(f * ND, ND)], load_sem.at[f]
        )
        for f in range(freq_dev)
    ]
    small = [
        pltpu.make_async_copy(sea_in, sea_raw, aux_sem.at[0]),
        pltpu.make_async_copy(wind_in, wind_raw, aux_sem.at[1]),
        pltpu.make_async_copy(angle_in, angle_raw, aux_sem.at[2]),
    ]
    for load in small[:1] + loads + small[1:]:
        load.start()

    @pl.when(zone == 0)
    def _():
        held[0:HALO] = jnp.zeros((HALO, ND, width), f32)

    @pl.when(zone == zones - 1)
    def _():
        held[HALO + freq_group :] = jnp.zeros((HALO, ND, width), f32)

    dirs = lax.broadcasted_iota(jnp.int32, (ND, LANES), 0).astype(f32)
    heading = 2.0 * math.pi * (dirs + 0.5) / ND
    cos_h, sin_h = jnp.cos(heading), jnp.sin(heading)
    log_step = math.log(1.1)
    lats = [math.radians(-75.0 + 150.0 * (r + 0.5) / lat_count) for r in range(lat_count)]
    small[0].wait()
    aux_ref[...] = sea_raw[...].astype(f32).reshape(1, cells)
    sea = [aux_ref[0:1, r * NLON : (r + 1) * NLON] for r in range(lat_count)]
    quarter = ND // 4
    tiles = NLON // LANES
    moments = [[jnp.zeros((quarter, NLON), f32) for _ in range(lat_count)] for _ in range(2)]
    for f in range(freq_dev):
        loads[f].wait()
        freq = (me * freq_dev + f).astype(f32)
        speed = 0.2 * jnp.exp(jnp.full((quarter, LANES), -log_step, f32) * freq)
        omega = jnp.exp(jnp.full((quarter, LANES), log_step, f32) * (freq - NF // 2))
        omega = jnp.concatenate([omega] * tiles, axis=1)
        sums = [None] * lat_count
        for q in range(4):
            east, north = q in (0, 3), q in (0, 1)
            rows = slice(f * ND + q * quarter, f * ND + (q + 1) * quarter)
            part = slice(q * quarter, (q + 1) * quarter)
            cx0 = speed * jnp.abs(cos_h[part])
            cy = jnp.concatenate([speed * jnp.abs(sin_h[part])] * tiles, axis=1)
            cx = [jnp.concatenate([cx0 * (1.0 / math.cos(a))] * tiles, axis=1) for a in lats]
            energy = [raw[rows, r * NLON : (r + 1) * NLON] * sea[r] for r in range(lat_count)]
            for _ in range(ADV_STEPS):
                fresh = []
                for r in range(lat_count):
                    e = energy[r]
                    side_x = pltpu.roll(e, 1 if east else NLON - 1, 1)
                    other = r - 1 if north else r + 1
                    side_y = energy[other] if 0 <= other < lat_count else 0.0
                    fresh.append((e - cx[r] * (e - side_x) - cy * (e - side_y)) * sea[r])
                energy = fresh
            for r in range(lat_count):
                adv[rows, r * NLON : (r + 1) * NLON] = energy[r]
                sums[r] = energy[r] if q == 0 else sums[r] + energy[r]
        for r in range(lat_count):
            moments[0][r] = moments[0][r] + sums[r]
            moments[1][r] = moments[1][r] + omega * sums[r]
    for i in range(2):
        for r in range(lat_count):
            mom_out[i : i + 1, r * NLON : (r + 1) * NLON] = jnp.sum(
                moments[i][r], axis=0, keepdims=True
            )

    pl.semaphore_wait(barrier, count - 1)

    def cells_of(index):
        return pl.ds(pl.multiple_of(index * width, LANES), width)

    for step in range(1, count):
        target = (me + step) % count
        remote(
            mom_out.at[:, cells_of(target % group)], mom_in.at[me],
            mom_send.at[step - 1], mom_recv.at[me], target,
        ).start()

    offsets = [(dy, dc) for dy in range(sides) for dc in range(2)]

    def rank_of(offset):
        return (side + offset[0]) % sides * 2 + (core + offset[1]) % 2

    def y_copy(f, i):
        peer = rank_of(offsets[i])
        return remote(
            adv.at[pl.ds(f * ND, ND), cells_of(peer)], held.at[HALO + rank * freq_dev + f],
            y_sem.at[i - 1, f], held_sem.at[HALO + rank * freq_dev + f], zone * group + peer,
        )

    def own_copy(f):
        slot = HALO + rank * freq_dev + f
        return pltpu.make_async_copy(
            adv.at[pl.ds(f * ND, ND), cells_of(rank)], held.at[slot], held_sem.at[slot]
        )

    for f in range(freq_dev):
        for i in list(range(2, group)) + [1]:
            y_copy(f, i).start()
        own_copy(f).start()
    local_mom = pltpu.make_async_copy(
        mom_out.at[:, cells_of(rank)], mom_in.at[me], mom_recv.at[me]
    )
    local_mom.start()

    small[1].wait()
    small[2].wait()
    speed_own = wind_raw[cells_of(rank)].reshape(1, width)
    angle_own = angle_raw[cells_of(rank)].reshape(1, width)
    wind[...] = jnp.concatenate([cos_h] * (width // LANES), axis=1) * (
        speed_own * jnp.cos(angle_own)
    ) + jnp.concatenate([sin_h] * (width // LANES), axis=1) * (speed_own * jnp.sin(angle_own))

    def up_copy(slot):
        return remote(
            held.at[HALO + slot], held.at[HALO + slot - freq_group],
            up_sem.at[slot - (freq_group - HALO)], held_sem.at[HALO + slot - freq_group],
            (zone + 1) % zones * group + rank,
        )

    def down_copy(slot):
        return remote(
            held.at[HALO + slot], held.at[HALO + slot + freq_group],
            down_sem.at[slot], held_sem.at[HALO + slot + freq_group],
            (zone + zones - 1) % zones * group + rank,
        )

    def arrive(index):
        remote(
            held.at[index], held.at[index], up_sem.at[0], held_sem.at[index],
            (me + 1) % count,
        ).wait_recv()

    for dy in range(sides):
        for f in range(freq_dev):
            for dc in range(2):
                slot = rank_of((dy, dc)) * freq_dev + f
                if (dy, dc) == (0, 0):
                    own_copy(f).wait()
                else:
                    arrive(HALO + slot)

                @pl.when((slot >= freq_group - HALO) & (zone < zones - 1))
                def _():
                    up_copy(slot).start()

                @pl.when((slot < HALO) & (zone > 0))
                def _():
                    down_copy(slot).start()

    local_mom.wait()
    for step in range(1, count):
        source = (me + step) % count
        remote(
            mom_in.at[source], mom_in.at[source], mom_send.at[0], mom_recv.at[source], source
        ).wait_recv()
    total = jnp.sum(mom_in[...], axis=0) * (1.0 / (NF * ND))
    energy_mean, moment_one = total[0:1], total[1:2]
    mean_freq = moment_one / (energy_mean + 1e-06)
    steepness = energy_mean * mean_freq * mean_freq
    breaking = steepness * steepness / (1.0 + steepness * steepness)

    acc[...] = jnp.zeros_like(acc)
    ascending = side > 0

    for i in range(HALO):
        early = jnp.where(ascending, i, HALO + freq_group + i)

        @pl.when(jnp.where(ascending, zone > 0, zone < zones - 1))
        def _():
            arrive(early)

    def ret_copy(k):
        owner, f = k // freq_dev, k % freq_dev
        return remote(
            done.at[k],
            out_ref.at[pl.ds(pl.multiple_of(f * ND, ND), ND), cells_of(rank)],
            ret_send.at[k], ret_recv.at[rank, f], zone * group + owner,
        )

    def ret_local(k):
        f = k % freq_dev
        return pltpu.make_async_copy(
            done.at[k],
            out_ref.at[pl.ds(pl.multiple_of(f * ND, ND), ND), cells_of(rank)],
            ret_recv.at[rank, f],
        )

    def source_step(i, carry):
        k = jnp.where(ascending, i, freq_group - 1 - i)
        late = i - (freq_group - HALO)

        @pl.when((late >= 0) & jnp.where(ascending, zone < zones - 1, zone > 0))
        def _():
            arrive(jnp.where(ascending, HALO + freq_group + late, HALO - 1 - late))

        freq = zone * freq_group + k

        def scale(index, factor):
            return jnp.where((index >= 3) & (index <= NF - 3), factor, 0.0).astype(f32)

        w_own, w_low, w_high = scale(freq, -0.002), scale(freq - 2, 0.001), scale(freq + 3, 0.001)
        omega = jnp.exp(
            jnp.full((1, LANES), log_step, f32) * (freq.astype(f32) - NF // 2)
        )
        for t in range(width // LANES):
            lanes = slice(t * LANES, (t + 1) * LANES)

            def slab(shift):
                return held[HALO + k + shift, :, lanes]

            def turn(values, amount):
                return pltpu.roll(values, amount % ND, 0)

            def rate(a, p, m):
                return a * (a * (p + m) - 2.0 * (p * m))

            own = slab(0)
            p2, m3, m2, m5, p3, p5 = (slab(s) for s in (2, -3, -2, -5, 3, 5))
            near = rate(own, turn(p2, -1), turn(m3, 3)) + rate(own, turn(p2, 1), turn(m3, -3))
            low = rate(turn(m2, 1), own, turn(m5, 4)) + rate(turn(m2, -1), own, turn(m5, -4))
            high = rate(turn(p3, -3), turn(p5, -4), own) + rate(turn(p3, 3), turn(p5, 4), own)
            interaction = w_own * near + w_low * low + w_high * high
            gain = (0.05 * omega) * jnp.maximum(0.0, wind[:, lanes] * omega - 1.0)
            damping = (0.03 * omega) * breaking[:, lanes]
            fresh = own + (gain - damping) * own + interaction
            done[k, :, lanes] = fresh
            acc[:, lanes] += fresh

        @pl.when(k // freq_dev == rank)
        def _():
            ret_local(k).start()

        @pl.when(k // freq_dev != rank)
        def _():
            ret_copy(k).start()

        return carry

    lax.fori_loop(0, freq_group, source_step, 0)

    sum_out[...] = jnp.sum(acc[...], axis=0, keepdims=True)

    def sum_copy(step):
        return remote(
            sum_out, sum_in.at[me], sum_send.at[step - 1], sum_recv.at[me], (me + step) % count
        )

    for step in range(1, count):
        sum_copy(step).start()
    sum_in[me] = sum_out[...]
    for step in range(1, count):
        source = (me + step) % count
        remote(
            sum_out, sum_in.at[source], sum_send.at[0], sum_recv.at[source], source
        ).wait_recv()

    per_row = count // group
    mine_row = me // per_row
    height_sum = jnp.zeros((1, width), f32)
    mine = jnp.zeros((1, width), f32)
    for g in range(group):
        mass = sum_in[g]
        for other in range(1, zones):
            mass = mass + sum_in[other * group + g]
        sea_row = aux_ref[0:1, g * width : (g + 1) * width]
        height = sea_row * (4.0 * jnp.sqrt(mass * (1.0 / (NF * ND)) + 1e-06))
        height_sum = height_sum + height
        mine = jnp.where(mine_row == g, height, mine)
    points = cells // count
    shift = (me % per_row) * points
    turned = pltpu.roll(jnp.broadcast_to(mine, (8, width)), (width - shift) % width, 1)
    wave_ref[...] = turned[0, :points]
    mean_ref[...] = jnp.sum(height_sum, axis=1, keepdims=True) * (1.0 / (SEA_DEV * count))

    for f in range(freq_dev):
        for i in range(1, group):
            peer = rank_of(offsets[i])
            remote(
                done.at[0], out_ref.at[pl.ds(f * ND, ND), cells_of(peer)],
                ret_send.at[0], ret_recv.at[peer, f], zone * group + peer,
            ).wait_recv()
            y_copy(f, i).wait_send()
            ret_copy(peer * freq_dev + f).wait_send()
        ret_local(rank * freq_dev + f).wait()
    for step in range(1, count):
        remote(
            mom_out.at[:, cells_of(0)], mom_in.at[me], mom_send.at[step - 1],
            mom_recv.at[me], (me + step) % count,
        ).wait_send()
        sum_copy(step).wait_send()

    @pl.when(zone < zones - 1)
    def _():
        for slot in range(freq_group - HALO, freq_group):
            up_copy(slot).wait_send()

    @pl.when(zone > 0)
    def _():
        for slot in range(HALO):
            down_copy(slot).wait_send()


def fused_local(spectrum, sea_mask, wind_speed, wind_angle):
    count = lax.axis_size("spec")
    bins_dev, cells = spectrum.shape
    group = group_size(count, bins_dev, cells)
    freq_dev = bins_dev // ND
    freq_group = freq_dev * group
    width = cells // group
    points = cells // count
    f32 = jnp.float32
    dma = pltpu.SemaphoreType.DMA
    out, wave, mean = pl.pallas_call(
        functools.partial(fused_kernel, count, group),
        out_shape=(
            pltpu.VMEM((bins_dev, cells), f32),
            pltpu.VMEM((points,), f32),
            jax.ShapeDtypeStruct((1, 1), f32),
        ),
        in_specs=[
            pl.BlockSpec(memory_space=pl.ANY),
        ]
        * 4,
        out_specs=(
            pl.BlockSpec(memory_space=pltpu.VMEM),
            pl.BlockSpec(memory_space=pltpu.VMEM),
            pl.BlockSpec(memory_space=pltpu.VMEM),
        ),
        scratch_shapes=[
            pltpu.VMEM((cells,), jnp.int32),
            pltpu.VMEM((cells,), f32),
            pltpu.VMEM((cells,), f32),
            pltpu.VMEM((1, cells), f32),
            dma((3,)),
            pltpu.VMEM((bins_dev, cells), f32),
            pltpu.VMEM((bins_dev, cells), f32),
            pltpu.VMEM((freq_group + 2 * HALO, ND, width), f32),
            pltpu.VMEM((freq_group, ND, width), f32),
            pltpu.VMEM((2, cells), f32),
            pltpu.VMEM((count, 2, width), f32),
            pltpu.VMEM((ND, width), f32),
            pltpu.VMEM((ND, width), f32),
            pltpu.VMEM((1, width), f32),
            pltpu.VMEM((count, 1, width), f32),
            dma((freq_dev,)),
            dma((freq_group + 2 * HALO,)),
            dma((group - 1, freq_dev)),
            dma((HALO,)),
            dma((HALO,)),
            dma((count - 1,)),
            dma((count,)),
            dma((freq_group,)),
            dma((group, freq_dev)),
            dma((count - 1,)),
            dma((count,)),
        ],
        compiler_params=pltpu.CompilerParams(collective_id=0, has_side_effects=True),
    )(sea_mask, wind_speed, wind_angle, spectrum)
    return (out, wave, mean.reshape(1))


def solution(mesh):
    in_specs = (P(("grp", "spec"), None), P(), P("grp"), P("grp"))
    out_specs = (P(("grp", "spec"), None), P(("grp", "spec")), P("grp"))

    def body(spectrum, sea_mask, wind_speed, wind_angle):
        fits = group_size(mesh.shape["spec"], *spectrum.shape)
        plan = fused_local if fits else local
        return plan(spectrum, sea_mask, wind_speed, wind_angle)

    return jax.shard_map(body, mesh=mesh, in_specs=in_specs, out_specs=out_specs, check_vma=False)
```

```python
import functools
import math

import jax
import jax.numpy as jnp
from jax import lax
from jax.experimental import pallas as pl
from jax.experimental.pallas import tpu as pltpu
from jax.sharding import PartitionSpec as P

NF = 48
ND = 32
NLON = 384
ADV_STEPS = 2
SEA_DEV = 64


def upwind_step(energy, courant_x, courant_y, sea_grid):
    west_cell = jnp.roll(energy, 1, axis=2)
    east_cell = jnp.roll(energy, -1, axis=2)
    edge_row = jnp.zeros_like(energy[:, :1])
    south_cell = jnp.concatenate([edge_row, energy[:, :-1]], axis=1)
    north_cell = jnp.concatenate([energy[:, 1:], edge_row], axis=1)
    updated = (
        energy
        - jnp.maximum(courant_x, 0.0) * (energy - west_cell)
        - jnp.minimum(courant_x, 0.0) * (east_cell - energy)
        - jnp.maximum(courant_y, 0.0) * (energy - south_cell)
        - jnp.minimum(courant_y, 0.0) * (north_cell - energy)
    )
    return updated * sea_grid


def courant_numbers(freq_index, dir_index, lat_count, dir_count):
    speed = 0.2 * jnp.exp(-math.log(1.1) * freq_index)
    heading = 2.0 * math.pi * (dir_index + 0.5) / dir_count
    rows = jnp.arange(lat_count, dtype=jnp.float32)
    latitude = (-75.0 + 150.0 * (rows + 0.5) / lat_count) * (math.pi / 180.0)
    courant_x = (speed * jnp.cos(heading))[:, None, None] / jnp.cos(latitude)[None, :, None]
    courant_y = (speed * jnp.sin(heading))[:, None, None]
    return (courant_x, courant_y)


def shift_freq(values, amount):
    if amount > 0:
        filler = jnp.zeros_like(values[:amount])
        return jnp.concatenate([filler, values[:-amount]], axis=0)
    filler = jnp.zeros_like(values[:-amount])
    return jnp.concatenate([values[-amount:], filler], axis=0)


def source_terms(energy, speed, angle):
    freq_count = energy.shape[0]
    dir_count = energy.shape[1]
    freq_ids = jnp.arange(freq_count, dtype=jnp.float32)
    frequency = jnp.exp(math.log(1.1) * (freq_ids - freq_count // 2))[:, None, None]
    heading = (2.0 * math.pi * (jnp.arange(dir_count, dtype=jnp.float32) + 0.5) / dir_count)[
        None, :, None
    ]
    energy_mean = jnp.mean(energy, axis=(0, 1))
    moment_one = jnp.mean(frequency * energy, axis=(0, 1))
    mean_freq = moment_one / (energy_mean + 1e-06)
    steepness = energy_mean * mean_freq * mean_freq
    breaking = steepness * steepness / (1.0 + steepness * steepness)
    wind_gain = (
        0.05
        * frequency
        * jnp.maximum(
            0.0, speed[None, None, :] * frequency * jnp.cos(heading - angle[None, None, :]) - 1.0
        )
    )
    damping = 0.03 * frequency * breaking[None, None, :]
    valid = ((freq_ids >= 3) & (freq_ids <= freq_count - 3)).astype(jnp.float32)[:, None, None]
    interaction = jnp.zeros_like(energy)
    for mirror in (1, -1):
        plus_bins = shift_freq(jnp.roll(energy, -mirror, axis=1), -2)
        minus_bins = shift_freq(jnp.roll(energy, 3 * mirror, axis=1), 3)
        transfer_rate = (
            0.001
            * valid
            * (energy * energy * (plus_bins + minus_bins) - 2.0 * energy * plus_bins * minus_bins)
        )
        interaction = interaction - 2.0 * transfer_rate
        interaction = interaction + jnp.roll(shift_freq(transfer_rate, 2), mirror, axis=1)
        interaction = interaction + jnp.roll(shift_freq(transfer_rate, -3), -3 * mirror, axis=1)
    updated = energy + (wind_gain - damping) * energy + interaction
    raw_height = 4.0 * jnp.sqrt(jnp.mean(updated, axis=(0, 1)) + 1e-06)
    return (updated, raw_height)


def local(spectrum, sea_mask, wind_speed, wind_angle):
    count = lax.axis_size("spec")
    position = lax.axis_index("spec")
    bins_dev = spectrum.shape[0]
    cells = spectrum.shape[1]
    points = cells // count
    lat_count = cells // NLON
    sea_float = sea_mask.astype(jnp.float32)
    bin_ids = position * bins_dev + jnp.arange(bins_dev, dtype=jnp.int32)
    freq_index = (bin_ids // ND).astype(jnp.float32)
    dir_index = (bin_ids % ND).astype(jnp.float32)
    courant_x, courant_y = courant_numbers(freq_index, dir_index, lat_count, ND)
    sea_grid = sea_float.reshape(1, lat_count, NLON)
    energy = (spectrum * sea_float[None, :]).reshape(bins_dev, lat_count, NLON)
    for substep in range(ADV_STEPS):
        energy = upwind_step(energy, courant_x, courant_y, sea_grid)
    advected = energy.reshape(bins_dev, cells)
    outgoing = advected.reshape(bins_dev, count, points)
    arrived = lax.all_to_all(outgoing, "spec", split_axis=1, concat_axis=0, tiled=True)
    start = position * points
    speed_own = lax.dynamic_slice_in_dim(wind_speed, start, points)
    angle_own = lax.dynamic_slice_in_dim(wind_angle, start, points)
    sea_own = lax.dynamic_slice_in_dim(sea_float, start, points)
    updated, raw_height = source_terms(arrived.reshape(NF, ND, points), speed_own, angle_own)
    wave_height = sea_own * raw_height
    own_total = jnp.zeros((count, 1), jnp.float32) + jnp.sum(wave_height)
    returned, totals = (
        lax.all_to_all(
            updated.reshape(NF * ND, 1, points), "spec", split_axis=0, concat_axis=1, tiled=True
        ),
        lax.all_to_all(own_total, "spec", split_axis=0, concat_axis=1, tiled=True),
    )
    new_spectrum = returned.reshape(bins_dev, cells)
    height_sum = jnp.sum(totals)
    mean_height = (height_sum / (SEA_DEV * count)).reshape(1)
    return (new_spectrum, wave_height, mean_height)


HALO = 5
LANES = 128


def group_size(count, bins_dev, cells):
    size = 4
    if count % size or bins_dev % ND or cells % (size * LANES) or cells % NLON:
        return 0
    if NLON % LANES or bins_dev // ND * size < 2 * HALO or cells % count:
        return 0
    return size


def fused_kernel(
    count, group, sea_in, wind_in, angle_in, spec_ref, out_ref, wave_ref, mean_ref,
    sea_raw, wind_raw, angle_raw, aux_ref, aux_sem,
    raw, adv, held, done, mom_out, mom_in, wind, acc, sum_out, sum_in,
    load_sem, held_sem, y_sem, up_sem, down_sem, mom_send, mom_recv,
    ret_send, ret_recv, sum_send, sum_recv,
):
    f32 = jnp.float32
    freq_dev, _, cells = adv.shape
    freq_group = freq_dev * group
    width = cells // group
    zones = count // group
    lat_count = cells // NLON
    sides = group // 2
    me = lax.axis_index("spec")
    zone, rank = me // group, me % group
    side, core = rank // 2, rank % 2

    def remote(src, dst, send, recv, target):
        return pltpu.make_async_remote_copy(
            src_ref=src, dst_ref=dst, send_sem=send, recv_sem=recv,
            device_id={"spec": target}, device_id_type=pl.DeviceIdType.MESH,
        )

    barrier = pltpu.get_barrier_semaphore()
    for step in range(1, count):
        pl.semaphore_signal(
            barrier, inc=1, device_id={"spec": (me + step) % count},
            device_id_type=pl.DeviceIdType.MESH,
        )
    loads = [
        pltpu.make_async_copy(
            spec_ref.at[pl.ds(f * ND, ND)], raw.at[pl.ds(f * ND, ND)], load_sem.at[f]
        )
        for f in range(freq_dev)
    ]
    small = [
        pltpu.make_async_copy(sea_in, sea_raw, aux_sem.at[0]),
        pltpu.make_async_copy(wind_in, wind_raw, aux_sem.at[1]),
        pltpu.make_async_copy(angle_in, angle_raw, aux_sem.at[2]),
    ]
    for load in small[:1] + loads + small[1:]:
        load.start()

    @pl.when(zone == 0)
    def _():
        held[0:HALO] = jnp.zeros((HALO, ND, width), f32)

    @pl.when(zone == zones - 1)
    def _():
        held[HALO + freq_group :] = jnp.zeros((HALO, ND, width), f32)

    def cells_of(index):
        return pl.ds(pl.multiple_of(index * width, LANES), width)

    def tile_of(index, t):
        return pl.ds(pl.multiple_of(index * width + t * LANES, LANES), LANES)

    def lanes_of(t):
        return pl.ds(t * LANES, LANES)

    offsets = [(dy, dc) for dy in range(sides) for dc in range(2)]

    def rank_of(offset):
        return (side + offset[0]) % sides * 2 + (core + offset[1]) % 2

    def y_copy(f, i, t):
        peer = rank_of(offsets[i])
        slot = HALO + rank * freq_dev + f
        return remote(
            adv.at[f, :, tile_of(peer, t)], held.at[slot, :, lanes_of(t)],
            y_sem.at[i - 1, f, t], held_sem.at[slot, t], zone * group + peer,
        )

    def own_copy(f, t):
        slot = HALO + rank * freq_dev + f
        return pltpu.make_async_copy(
            adv.at[f, :, tile_of(rank, t)], held.at[slot, :, lanes_of(t)], held_sem.at[slot, t]
        )

    def y_start(f, t):
        for i in list(range(2, group)) + [1]:
            y_copy(f, i, t).start()
        own_copy(f, t).start()

    dirs = lax.broadcasted_iota(jnp.int32, (ND, LANES), 0).astype(f32)
    heading = 2.0 * math.pi * (dirs + 0.5) / ND
    cos_h, sin_h = jnp.cos(heading), jnp.sin(heading)
    log_step = math.log(1.1)
    lats = [math.radians(-75.0 + 150.0 * (r + 0.5) / lat_count) for r in range(lat_count)]
    small[0].wait()
    aux_ref[...] = sea_raw[...].astype(f32).reshape(1, cells)
    sea = [aux_ref[0:1, r * NLON : (r + 1) * NLON] for r in range(lat_count)]
    quarter = ND // 4
    tiles = NLON // LANES
    parts = width // LANES
    moments = [[jnp.zeros((quarter, NLON), f32) for _ in range(lat_count)] for _ in range(2)]
    for f in range(freq_dev):
        loads[f].wait()
        freq = (me * freq_dev + f).astype(f32)
        speed = 0.2 * jnp.exp(jnp.full((quarter, LANES), -log_step, f32) * freq)
        omega = jnp.exp(jnp.full((quarter, LANES), log_step, f32) * (freq - NF // 2))
        omega = jnp.concatenate([omega] * tiles, axis=1)
        sums = [None] * lat_count
        for q in range(4):
            east, north = q in (0, 3), q in (0, 1)
            rows = slice(f * ND + q * quarter, f * ND + (q + 1) * quarter)
            part = slice(q * quarter, (q + 1) * quarter)
            cx0 = speed * jnp.abs(cos_h[part])
            cy = jnp.concatenate([speed * jnp.abs(sin_h[part])] * tiles, axis=1)
            cx = [jnp.concatenate([cx0 * (1.0 / math.cos(a))] * tiles, axis=1) for a in lats]
            energy = [raw[rows, r * NLON : (r + 1) * NLON] * sea[r] for r in range(lat_count)]
            for _ in range(ADV_STEPS):
                fresh = []
                for r in range(lat_count):
                    e = energy[r]
                    side_x = pltpu.roll(e, 1 if east else NLON - 1, 1)
                    other = r - 1 if north else r + 1
                    side_y = energy[other] if 0 <= other < lat_count else 0.0
                    fresh.append((e - cx[r] * (e - side_x) - cy * (e - side_y)) * sea[r])
                energy = fresh
            for r in range(lat_count):
                adv[f, part, r * NLON : (r + 1) * NLON] = energy[r]
                sums[r] = energy[r] if q == 0 else sums[r] + energy[r]
        for r in range(lat_count):
            moments[0][r] = moments[0][r] + sums[r]
            moments[1][r] = moments[1][r] + omega * sums[r]
        if f == 0:
            pl.semaphore_wait(barrier, count - 1)
        if f < freq_dev - 1:
            y_start(f, 0)
    for i in range(2):
        for r in range(lat_count):
            mom_out[i : i + 1, r * NLON : (r + 1) * NLON] = jnp.sum(
                moments[i][r], axis=0, keepdims=True
            )

    for step in range(1, count):
        target = (me + step) % count
        remote(
            mom_out.at[:, cells_of(target % group)], mom_in.at[me],
            mom_send.at[step - 1], mom_recv.at[me], target,
        ).start()
    local_mom = pltpu.make_async_copy(
        mom_out.at[:, cells_of(rank)], mom_in.at[me], mom_recv.at[me]
    )
    local_mom.start()
    y_start(freq_dev - 1, 0)
    for t in range(1, parts):
        for f in range(freq_dev):
            y_start(f, t)

    small[1].wait()
    small[2].wait()
    speed_own = wind_raw[cells_of(rank)].reshape(1, width)
    angle_own = angle_raw[cells_of(rank)].reshape(1, width)
    wind[...] = jnp.concatenate([cos_h] * (width // LANES), axis=1) * (
        speed_own * jnp.cos(angle_own)
    ) + jnp.concatenate([sin_h] * (width // LANES), axis=1) * (speed_own * jnp.sin(angle_own))

    def up_copy(slot, t):
        return remote(
            held.at[HALO + slot, :, lanes_of(t)],
            held.at[HALO + slot - freq_group, :, lanes_of(t)],
            up_sem.at[slot - (freq_group - HALO), t],
            held_sem.at[HALO + slot - freq_group, t],
            (zone + 1) % zones * group + rank,
        )

    def down_copy(slot, t):
        return remote(
            held.at[HALO + slot, :, lanes_of(t)],
            held.at[HALO + slot + freq_group, :, lanes_of(t)],
            down_sem.at[slot, t],
            held_sem.at[HALO + slot + freq_group, t],
            (zone + zones - 1) % zones * group + rank,
        )

    def arrive(index, t):
        block = held.at[index, :, lanes_of(t)]
        remote(
            block, block, up_sem.at[0, t], held_sem.at[index, t], (me + 1) % count
        ).wait_recv()

    def arrive_group(dy, t):
        for f in range(freq_dev):
            for dc in range(2):
                slot = rank_of((dy, dc)) * freq_dev + f
                if (dy, dc) == (0, 0):
                    own_copy(f, t).wait()
                else:
                    arrive(HALO + slot, t)

                @pl.when((slot >= freq_group - HALO) & (zone < zones - 1))
                def _():
                    up_copy(slot, t).start()

                @pl.when((slot < HALO) & (zone > 0))
                def _():
                    down_copy(slot, t).start()

    for t in range(parts):
        arrive_group(0, t)
    for dy in range(1, sides):
        arrive_group(dy, 0)

    local_mom.wait()
    for step in range(1, count):
        source = (me + step) % count
        remote(
            mom_in.at[source], mom_in.at[source], mom_send.at[0], mom_recv.at[source], source
        ).wait_recv()
    total = jnp.sum(mom_in[...], axis=0) * (1.0 / (NF * ND))
    energy_mean, moment_one = total[0:1], total[1:2]
    mean_freq = moment_one / (energy_mean + 1e-06)
    steepness = energy_mean * mean_freq * mean_freq
    breaking = steepness * steepness / (1.0 + steepness * steepness)

    acc[...] = jnp.zeros_like(acc)
    ascending = side > 0

    def arrive_halo(at_top, t):
        @pl.when(jnp.where(at_top, zone < zones - 1, zone > 0))
        def _():
            for i in range(HALO):
                arrive(jnp.where(at_top, HALO + freq_group + i, i), t)

    def ret_copy(owner, t):
        return remote(
            done.at[pl.ds(owner * freq_dev, freq_dev), :, lanes_of(t)],
            out_ref.at[:, :, tile_of(rank, t)],
            ret_send.at[owner, t], ret_recv.at[rank, t], zone * group + owner,
        )

    def ret_local(t):
        return pltpu.make_async_copy(
            done.at[pl.ds(rank * freq_dev, freq_dev), :, lanes_of(t)],
            out_ref.at[:, :, tile_of(rank, t)],
            ret_recv.at[rank, t],
        )

    def sources(t, begin, end):
        lanes = slice(t * LANES, (t + 1) * LANES)

        def source_step(i, carry):
            k = jnp.where(ascending, i, freq_group - 1 - i)
            freq = zone * freq_group + k

            def scale(index, factor):
                return jnp.where((index >= 3) & (index <= NF - 3), factor, 0.0).astype(f32)

            w_own = scale(freq, -0.002)
            w_low, w_high = scale(freq - 2, 0.001), scale(freq + 3, 0.001)
            omega = jnp.exp(
                jnp.full((1, LANES), log_step, f32) * (freq.astype(f32) - NF // 2)
            )

            def slab(shift):
                return held[HALO + k + shift, :, lanes]

            def turn(values, amount):
                return pltpu.roll(values, amount % ND, 0)

            def rate(a, p, m):
                return a * (a * (p + m) - 2.0 * (p * m))

            own = slab(0)
            p2, m3, m2, m5, p3, p5 = (slab(shift) for shift in (2, -3, -2, -5, 3, 5))
            near = rate(own, turn(p2, -1), turn(m3, 3)) + rate(own, turn(p2, 1), turn(m3, -3))
            low = rate(turn(m2, 1), own, turn(m5, 4)) + rate(turn(m2, -1), own, turn(m5, -4))
            high = rate(turn(p3, -3), turn(p5, -4), own) + rate(turn(p3, 3), turn(p5, 4), own)
            interaction = w_own * near + w_low * low + w_high * high
            gain = (0.05 * omega) * jnp.maximum(0.0, wind[:, lanes] * omega - 1.0)
            damping = (0.03 * omega) * breaking[:, lanes]
            fresh = own + (gain - damping) * own + interaction
            done[k, :, lanes] = fresh
            acc[:, lanes] += fresh
            return carry

        lax.fori_loop(begin, end, source_step, 0)

    half = freq_group // 2
    near_side = rank_of((0, 1))

    def first_half(t):
        arrive_halo(jnp.logical_not(ascending), t)
        sources(t, 0, half)
        for dy in range(1, sides):
            for dc in range(2):
                ret_copy(rank_of((dy, dc)), t).start()

    def second_half(t):
        arrive_halo(ascending, t)
        sources(t, half, freq_group)
        ret_copy(near_side, t).start()
        ret_local(t).start()

    first_half(0)
    for t in range(1, parts):
        for dy in range(1, sides):
            arrive_group(dy, t)
        first_half(t)
        second_half(t - 1)
    second_half(parts - 1)

    sum_out[...] = jnp.sum(acc[...], axis=0, keepdims=True)

    def sum_copy(step):
        return remote(
            sum_out, sum_in.at[me], sum_send.at[step - 1], sum_recv.at[me], (me + step) % count
        )

    for step in range(1, count):
        sum_copy(step).start()
    sum_in[me] = sum_out[...]
    for step in range(1, count):
        source = (me + step) % count
        remote(
            sum_out, sum_in.at[source], sum_send.at[0], sum_recv.at[source], source
        ).wait_recv()

    per_row = count // group
    mine_row = me // per_row
    height_sum = jnp.zeros((1, width), f32)
    mine = jnp.zeros((1, width), f32)
    for g in range(group):
        mass = sum_in[g]
        for other in range(1, zones):
            mass = mass + sum_in[other * group + g]
        sea_row = aux_ref[0:1, g * width : (g + 1) * width]
        height = sea_row * (4.0 * jnp.sqrt(mass * (1.0 / (NF * ND)) + 1e-06))
        height_sum = height_sum + height
        mine = jnp.where(mine_row == g, height, mine)
    points = cells // count
    shift = (me % per_row) * points
    turned = pltpu.roll(jnp.broadcast_to(mine, (8, width)), (width - shift) % width, 1)
    wave_ref[...] = turned[0, :points]
    mean_ref[...] = jnp.sum(height_sum, axis=1, keepdims=True) * (1.0 / (SEA_DEV * count))

    for t in range(parts):
        for i in range(1, group):
            peer = rank_of(offsets[i])
            remote(
                done.at[pl.ds(0, freq_dev), :, lanes_of(t)], out_ref.at[:, :, tile_of(peer, t)],
                ret_send.at[peer, t], ret_recv.at[peer, t], zone * group + peer,
            ).wait_recv()
            for f in range(freq_dev):
                y_copy(f, i, t).wait_send()
            ret_copy(peer, t).wait_send()
        ret_local(t).wait()
    for step in range(1, count):
        remote(
            mom_out.at[:, cells_of(0)], mom_in.at[me], mom_send.at[step - 1],
            mom_recv.at[me], (me + step) % count,
        ).wait_send()
        sum_copy(step).wait_send()

    @pl.when(zone < zones - 1)
    def _():
        for t in range(parts):
            for slot in range(freq_group - HALO, freq_group):
                up_copy(slot, t).wait_send()

    @pl.when(zone > 0)
    def _():
        for t in range(parts):
            for slot in range(HALO):
                down_copy(slot, t).wait_send()


def fused_local(spectrum, sea_mask, wind_speed, wind_angle):
    count = lax.axis_size("spec")
    bins_dev, cells = spectrum.shape
    group = group_size(count, bins_dev, cells)
    freq_dev = bins_dev // ND
    freq_group = freq_dev * group
    width = cells // group
    points = cells // count
    parts = width // LANES
    f32 = jnp.float32
    dma = pltpu.SemaphoreType.DMA
    out, wave, mean = pl.pallas_call(
        functools.partial(fused_kernel, count, group),
        out_shape=(
            pltpu.VMEM((freq_dev, ND, cells), f32),
            pltpu.VMEM((points,), f32),
            jax.ShapeDtypeStruct((1, 1), f32),
        ),
        in_specs=[
            pl.BlockSpec(memory_space=pl.ANY),
        ]
        * 4,
        out_specs=(
            pl.BlockSpec(memory_space=pltpu.VMEM),
            pl.BlockSpec(memory_space=pltpu.VMEM),
            pl.BlockSpec(memory_space=pltpu.VMEM),
        ),
        scratch_shapes=[
            pltpu.VMEM((cells,), jnp.int32),
            pltpu.VMEM((cells,), f32),
            pltpu.VMEM((cells,), f32),
            pltpu.VMEM((1, cells), f32),
            dma((3,)),
            pltpu.VMEM((bins_dev, cells), f32),
            pltpu.VMEM((freq_dev, ND, cells), f32),
            pltpu.VMEM((freq_group + 2 * HALO, ND, width), f32),
            pltpu.VMEM((freq_group, ND, width), f32),
            pltpu.VMEM((2, cells), f32),
            pltpu.VMEM((count, 2, width), f32),
            pltpu.VMEM((ND, width), f32),
            pltpu.VMEM((ND, width), f32),
            pltpu.VMEM((1, width), f32),
            pltpu.VMEM((count, 1, width), f32),
            dma((freq_dev,)),
            dma((freq_group + 2 * HALO, parts)),
            dma((group - 1, freq_dev, parts)),
            dma((HALO, parts)),
            dma((HALO, parts)),
            dma((count - 1,)),
            dma((count,)),
            dma((group, parts)),
            dma((group, parts)),
            dma((count - 1,)),
            dma((count,)),
        ],
        compiler_params=pltpu.CompilerParams(collective_id=0, has_side_effects=True),
    )(sea_mask, wind_speed, wind_angle, spectrum)
    return (out.reshape(bins_dev, cells), wave, mean.reshape(1))


def solution(mesh):
    in_specs = (P(("grp", "spec"), None), P(), P("grp"), P("grp"))
    out_specs = (P(("grp", "spec"), None), P(("grp", "spec")), P("grp"))

    def body(spectrum, sea_mask, wind_speed, wind_angle):
        fits = group_size(mesh.shape["spec"], *spectrum.shape)
        plan = fused_local if fits else local
        return plan(spectrum, sea_mask, wind_speed, wind_angle)

    return jax.shard_map(body, mesh=mesh, in_specs=in_specs, out_specs=out_specs, check_vma=False)
```

```python
import functools
import math

import jax
import jax.numpy as jnp
from jax import lax
from jax.experimental import pallas as pl
from jax.experimental.pallas import tpu as pltpu
from jax.sharding import PartitionSpec as P

NF = 48
ND = 32
NLON = 384
ADV_STEPS = 2
SEA_DEV = 64


def upwind_step(energy, courant_x, courant_y, sea_grid):
    west_cell = jnp.roll(energy, 1, axis=2)
    east_cell = jnp.roll(energy, -1, axis=2)
    edge_row = jnp.zeros_like(energy[:, :1])
    south_cell = jnp.concatenate([edge_row, energy[:, :-1]], axis=1)
    north_cell = jnp.concatenate([energy[:, 1:], edge_row], axis=1)
    updated = (
        energy
        - jnp.maximum(courant_x, 0.0) * (energy - west_cell)
        - jnp.minimum(courant_x, 0.0) * (east_cell - energy)
        - jnp.maximum(courant_y, 0.0) * (energy - south_cell)
        - jnp.minimum(courant_y, 0.0) * (north_cell - energy)
    )
    return updated * sea_grid


def courant_numbers(freq_index, dir_index, lat_count, dir_count):
    speed = 0.2 * jnp.exp(-math.log(1.1) * freq_index)
    heading = 2.0 * math.pi * (dir_index + 0.5) / dir_count
    rows = jnp.arange(lat_count, dtype=jnp.float32)
    latitude = (-75.0 + 150.0 * (rows + 0.5) / lat_count) * (math.pi / 180.0)
    courant_x = (speed * jnp.cos(heading))[:, None, None] / jnp.cos(latitude)[None, :, None]
    courant_y = (speed * jnp.sin(heading))[:, None, None]
    return (courant_x, courant_y)


def shift_freq(values, amount):
    if amount > 0:
        filler = jnp.zeros_like(values[:amount])
        return jnp.concatenate([filler, values[:-amount]], axis=0)
    filler = jnp.zeros_like(values[:-amount])
    return jnp.concatenate([values[-amount:], filler], axis=0)


def source_terms(energy, speed, angle):
    freq_count = energy.shape[0]
    dir_count = energy.shape[1]
    freq_ids = jnp.arange(freq_count, dtype=jnp.float32)
    frequency = jnp.exp(math.log(1.1) * (freq_ids - freq_count // 2))[:, None, None]
    heading = (2.0 * math.pi * (jnp.arange(dir_count, dtype=jnp.float32) + 0.5) / dir_count)[
        None, :, None
    ]
    energy_mean = jnp.mean(energy, axis=(0, 1))
    moment_one = jnp.mean(frequency * energy, axis=(0, 1))
    mean_freq = moment_one / (energy_mean + 1e-06)
    steepness = energy_mean * mean_freq * mean_freq
    breaking = steepness * steepness / (1.0 + steepness * steepness)
    wind_gain = (
        0.05
        * frequency
        * jnp.maximum(
            0.0, speed[None, None, :] * frequency * jnp.cos(heading - angle[None, None, :]) - 1.0
        )
    )
    damping = 0.03 * frequency * breaking[None, None, :]
    valid = ((freq_ids >= 3) & (freq_ids <= freq_count - 3)).astype(jnp.float32)[:, None, None]
    interaction = jnp.zeros_like(energy)
    for mirror in (1, -1):
        plus_bins = shift_freq(jnp.roll(energy, -mirror, axis=1), -2)
        minus_bins = shift_freq(jnp.roll(energy, 3 * mirror, axis=1), 3)
        transfer_rate = (
            0.001
            * valid
            * (energy * energy * (plus_bins + minus_bins) - 2.0 * energy * plus_bins * minus_bins)
        )
        interaction = interaction - 2.0 * transfer_rate
        interaction = interaction + jnp.roll(shift_freq(transfer_rate, 2), mirror, axis=1)
        interaction = interaction + jnp.roll(shift_freq(transfer_rate, -3), -3 * mirror, axis=1)
    updated = energy + (wind_gain - damping) * energy + interaction
    raw_height = 4.0 * jnp.sqrt(jnp.mean(updated, axis=(0, 1)) + 1e-06)
    return (updated, raw_height)


def local(spectrum, sea_mask, wind_speed, wind_angle):
    count = lax.axis_size("spec")
    position = lax.axis_index("spec")
    bins_dev = spectrum.shape[0]
    cells = spectrum.shape[1]
    points = cells // count
    lat_count = cells // NLON
    sea_float = sea_mask.astype(jnp.float32)
    bin_ids = position * bins_dev + jnp.arange(bins_dev, dtype=jnp.int32)
    freq_index = (bin_ids // ND).astype(jnp.float32)
    dir_index = (bin_ids % ND).astype(jnp.float32)
    courant_x, courant_y = courant_numbers(freq_index, dir_index, lat_count, ND)
    sea_grid = sea_float.reshape(1, lat_count, NLON)
    energy = (spectrum * sea_float[None, :]).reshape(bins_dev, lat_count, NLON)
    for substep in range(ADV_STEPS):
        energy = upwind_step(energy, courant_x, courant_y, sea_grid)
    advected = energy.reshape(bins_dev, cells)
    outgoing = advected.reshape(bins_dev, count, points)
    arrived = lax.all_to_all(outgoing, "spec", split_axis=1, concat_axis=0, tiled=True)
    start = position * points
    speed_own = lax.dynamic_slice_in_dim(wind_speed, start, points)
    angle_own = lax.dynamic_slice_in_dim(wind_angle, start, points)
    sea_own = lax.dynamic_slice_in_dim(sea_float, start, points)
    updated, raw_height = source_terms(arrived.reshape(NF, ND, points), speed_own, angle_own)
    wave_height = sea_own * raw_height
    own_total = jnp.zeros((count, 1), jnp.float32) + jnp.sum(wave_height)
    returned, totals = (
        lax.all_to_all(
            updated.reshape(NF * ND, 1, points), "spec", split_axis=0, concat_axis=1, tiled=True
        ),
        lax.all_to_all(own_total, "spec", split_axis=0, concat_axis=1, tiled=True),
    )
    new_spectrum = returned.reshape(bins_dev, cells)
    height_sum = jnp.sum(totals)
    mean_height = (height_sum / (SEA_DEV * count)).reshape(1)
    return (new_spectrum, wave_height, mean_height)


HALO = 5
LANES = 128


def group_size(count, bins_dev, cells):
    size = 4
    if count % size or bins_dev % ND or cells % (size * LANES) or cells % NLON:
        return 0
    if NLON % LANES or bins_dev // ND * size < 2 * HALO or cells % count:
        return 0
    return size


def fused_kernel(
    count, group, sea_in, wind_in, angle_in, spec_ref, out_ref, wave_ref, mean_ref,
    sea_raw, wind_raw, angle_raw, aux_ref, aux_sem,
    raw, adv, held, done, mom_out, mom_in, wind, acc, sum_out, sum_in,
    load_sem, held_sem, y_sem, up_sem, down_sem, mom_send, mom_recv,
    ret_send, ret_recv, sum_send, sum_recv,
):
    f32 = jnp.float32
    freq_dev, _, cells = adv.shape
    freq_group = freq_dev * group
    width = cells // group
    zones = count // group
    lat_count = cells // NLON
    sides = group // 2
    me = lax.axis_index("spec")
    zone, rank = me // group, me % group
    side, core = rank // 2, rank % 2

    def remote(src, dst, send, recv, target):
        return pltpu.make_async_remote_copy(
            src_ref=src, dst_ref=dst, send_sem=send, recv_sem=recv,
            device_id={"spec": target}, device_id_type=pl.DeviceIdType.MESH,
        )

    barrier = pltpu.get_barrier_semaphore()
    for step in range(1, count):
        pl.semaphore_signal(
            barrier, inc=1, device_id={"spec": (me + step) % count},
            device_id_type=pl.DeviceIdType.MESH,
        )
    loads = [
        pltpu.make_async_copy(
            spec_ref.at[pl.ds(f * ND, ND)], raw.at[pl.ds(f * ND, ND)], load_sem.at[f]
        )
        for f in range(freq_dev)
    ]
    small = [
        pltpu.make_async_copy(sea_in, sea_raw, aux_sem.at[0]),
        pltpu.make_async_copy(wind_in, wind_raw, aux_sem.at[1]),
        pltpu.make_async_copy(angle_in, angle_raw, aux_sem.at[2]),
    ]
    for load in small[:1] + loads + small[1:]:
        load.start()

    @pl.when(zone == 0)
    def _():
        held[0:HALO] = jnp.zeros((HALO, ND, width), f32)

    @pl.when(zone == zones - 1)
    def _():
        held[HALO + freq_group :] = jnp.zeros((HALO, ND, width), f32)

    def cells_of(index):
        return pl.ds(pl.multiple_of(index * width, LANES), width)

    def tile_of(index, t):
        return pl.ds(pl.multiple_of(index * width + t * LANES, LANES), LANES)

    def lanes_of(t):
        return pl.ds(t * LANES, LANES)

    offsets = [(dy, dc) for dy in range(sides) for dc in range(2)]

    def rank_of(offset):
        return (side + offset[0]) % sides * 2 + (core + offset[1]) % 2

    def y_copy(f, i, t):
        peer = rank_of(offsets[i])
        slot = HALO + rank * freq_dev + f
        return remote(
            adv.at[f, :, tile_of(peer, t)], held.at[slot, :, lanes_of(t)],
            y_sem.at[i - 1, f, t], held_sem.at[slot, t], zone * group + peer,
        )

    def own_copy(f, t):
        slot = HALO + rank * freq_dev + f
        return pltpu.make_async_copy(
            adv.at[f, :, tile_of(rank, t)], held.at[slot, :, lanes_of(t)], held_sem.at[slot, t]
        )

    def y_start(f, t):
        for i in list(range(2, group)) + [1]:
            y_copy(f, i, t).start()
        own_copy(f, t).start()

    dirs = lax.broadcasted_iota(jnp.int32, (ND, LANES), 0).astype(f32)
    heading = 2.0 * math.pi * (dirs + 0.5) / ND
    cos_h, sin_h = jnp.cos(heading), jnp.sin(heading)
    log_step = math.log(1.1)
    lats = [math.radians(-75.0 + 150.0 * (r + 0.5) / lat_count) for r in range(lat_count)]
    small[0].wait()
    aux_ref[...] = sea_raw[...].astype(f32).reshape(1, cells)
    sea = [aux_ref[0:1, r * NLON : (r + 1) * NLON] for r in range(lat_count)]
    quarter = ND // 4
    tiles = NLON // LANES
    parts = width // LANES
    moments = [[jnp.zeros((quarter, NLON), f32) for _ in range(lat_count)] for _ in range(2)]
    for f in range(freq_dev):
        loads[f].wait()
        freq = (me * freq_dev + f).astype(f32)
        speed = 0.2 * jnp.exp(jnp.full((quarter, LANES), -log_step, f32) * freq)
        omega = jnp.exp(jnp.full((quarter, LANES), log_step, f32) * (freq - NF // 2))
        omega = jnp.concatenate([omega] * tiles, axis=1)
        sums = [None] * lat_count
        for q in range(4):
            east, north = q in (0, 3), q in (0, 1)
            rows = slice(f * ND + q * quarter, f * ND + (q + 1) * quarter)
            part = slice(q * quarter, (q + 1) * quarter)
            cx0 = speed * jnp.abs(cos_h[part])
            cy = jnp.concatenate([speed * jnp.abs(sin_h[part])] * tiles, axis=1)
            cx = [jnp.concatenate([cx0 * (1.0 / math.cos(a))] * tiles, axis=1) for a in lats]
            energy = [raw[rows, r * NLON : (r + 1) * NLON] * sea[r] for r in range(lat_count)]
            for _ in range(ADV_STEPS):
                fresh = []
                for r in range(lat_count):
                    e = energy[r]
                    side_x = pltpu.roll(e, 1 if east else NLON - 1, 1)
                    other = r - 1 if north else r + 1
                    side_y = energy[other] if 0 <= other < lat_count else 0.0
                    fresh.append((e - cx[r] * (e - side_x) - cy * (e - side_y)) * sea[r])
                energy = fresh
            for r in range(lat_count):
                adv[f, part, r * NLON : (r + 1) * NLON] = energy[r]
                sums[r] = energy[r] if q == 0 else sums[r] + energy[r]
        for r in range(lat_count):
            moments[0][r] = moments[0][r] + sums[r]
            moments[1][r] = moments[1][r] + omega * sums[r]
        if f == 0:
            pl.semaphore_wait(barrier, count - 1)
        if f < freq_dev - 1:
            y_start(f, 0)
    for i in range(2):
        for r in range(lat_count):
            mom_out[i : i + 1, r * NLON : (r + 1) * NLON] = jnp.sum(
                moments[i][r], axis=0, keepdims=True
            )

    for step in range(1, count):
        target = (me + step) % count
        remote(
            mom_out.at[:, cells_of(target % group)], mom_in.at[me],
            mom_send.at[step - 1], mom_recv.at[me], target,
        ).start()
    local_mom = pltpu.make_async_copy(
        mom_out.at[:, cells_of(rank)], mom_in.at[me], mom_recv.at[me]
    )
    local_mom.start()
    y_start(freq_dev - 1, 0)
    for t in range(1, parts):
        for f in range(freq_dev):
            y_start(f, t)

    small[1].wait()
    small[2].wait()
    speed_own = wind_raw[cells_of(rank)].reshape(1, width)
    angle_own = angle_raw[cells_of(rank)].reshape(1, width)
    wind[...] = jnp.concatenate([cos_h] * (width // LANES), axis=1) * (
        speed_own * jnp.cos(angle_own)
    ) + jnp.concatenate([sin_h] * (width // LANES), axis=1) * (speed_own * jnp.sin(angle_own))

    def up_copy(slot, t):
        return remote(
            held.at[HALO + slot, :, lanes_of(t)],
            held.at[HALO + slot - freq_group, :, lanes_of(t)],
            up_sem.at[slot - (freq_group - HALO), t],
            held_sem.at[HALO + slot - freq_group, t],
            (zone + 1) % zones * group + rank,
        )

    def down_copy(slot, t):
        return remote(
            held.at[HALO + slot, :, lanes_of(t)],
            held.at[HALO + slot + freq_group, :, lanes_of(t)],
            down_sem.at[slot, t],
            held_sem.at[HALO + slot + freq_group, t],
            (zone + zones - 1) % zones * group + rank,
        )

    def arrive(index, t):
        block = held.at[index, :, lanes_of(t)]
        remote(
            block, block, up_sem.at[0, t], held_sem.at[index, t], (me + 1) % count
        ).wait_recv()

    def arrive_group(dy, t):
        for f in range(freq_dev):
            for dc in range(2):
                slot = rank_of((dy, dc)) * freq_dev + f
                if (dy, dc) == (0, 0):
                    own_copy(f, t).wait()
                else:
                    arrive(HALO + slot, t)

                @pl.when((slot >= freq_group - HALO) & (zone < zones - 1))
                def _():
                    up_copy(slot, t).start()

                @pl.when((slot < HALO) & (zone > 0))
                def _():
                    down_copy(slot, t).start()

    for t in range(parts):
        arrive_group(0, t)
    for dy in range(1, sides):
        arrive_group(dy, 0)

    local_mom.wait()
    for step in range(1, count):
        source = (me + step) % count
        remote(
            mom_in.at[source], mom_in.at[source], mom_send.at[0], mom_recv.at[source], source
        ).wait_recv()
    total = jnp.sum(mom_in[...], axis=0) * (1.0 / (NF * ND))
    energy_mean, moment_one = total[0:1], total[1:2]
    mean_freq = moment_one / (energy_mean + 1e-06)
    steepness = energy_mean * mean_freq * mean_freq
    breaking = steepness * steepness / (1.0 + steepness * steepness)

    acc[...] = jnp.zeros_like(acc)
    ascending = side > 0

    def arrive_halo(at_top, t):
        @pl.when(jnp.where(at_top, zone < zones - 1, zone > 0))
        def _():
            for i in range(HALO):
                arrive(jnp.where(at_top, HALO + freq_group + i, i), t)

    def ret_copy(owner, t):
        return remote(
            done.at[pl.ds(owner * freq_dev, freq_dev), :, lanes_of(t)],
            out_ref.at[:, :, tile_of(rank, t)],
            ret_send.at[owner, t], ret_recv.at[rank, t], zone * group + owner,
        )

    def ret_local(t):
        return pltpu.make_async_copy(
            done.at[pl.ds(rank * freq_dev, freq_dev), :, lanes_of(t)],
            out_ref.at[:, :, tile_of(rank, t)],
            ret_recv.at[rank, t],
        )

    def sources(t, begin, end):
        lanes = slice(t * LANES, (t + 1) * LANES)

        def source_step(i, carry):
            k = jnp.where(ascending, i, freq_group - 1 - i)
            freq = zone * freq_group + k

            def scale(index, factor):
                return jnp.where((index >= 3) & (index <= NF - 3), factor, 0.0).astype(f32)

            w_own = scale(freq, -0.002)
            w_low, w_high = scale(freq - 2, 0.001), scale(freq + 3, 0.001)
            omega = jnp.exp(
                jnp.full((1, LANES), log_step, f32) * (freq.astype(f32) - NF // 2)
            )

            def slab(shift):
                return held[HALO + k + shift, :, lanes]

            def turn(values, amount):
                return pltpu.roll(values, amount % ND, 0)

            def rate(a, p, m):
                return a * (a * (p + m) - 2.0 * (p * m))

            own = slab(0)
            p2, m3, m2, m5, p3, p5 = (slab(shift) for shift in (2, -3, -2, -5, 3, 5))
            near = rate(own, turn(p2, -1), turn(m3, 3)) + rate(own, turn(p2, 1), turn(m3, -3))
            low = rate(turn(m2, 1), own, turn(m5, 4)) + rate(turn(m2, -1), own, turn(m5, -4))
            high = rate(turn(p3, -3), turn(p5, -4), own) + rate(turn(p3, 3), turn(p5, 4), own)
            interaction = w_own * near + w_low * low + w_high * high
            gain = (0.05 * omega) * jnp.maximum(0.0, wind[:, lanes] * omega - 1.0)
            damping = (0.03 * omega) * breaking[:, lanes]
            fresh = own + (gain - damping) * own + interaction
            done[k, :, lanes] = fresh
            acc[:, lanes] += fresh
            return carry

        lax.fori_loop(begin, end, source_step, 0)

    half = freq_group // 2
    near_side = rank_of((0, 1))

    def first_half(t):
        arrive_halo(jnp.logical_not(ascending), t)
        sources(t, 0, half)
        for dy in range(1, sides):
            for dc in range(2):
                ret_copy(rank_of((dy, dc)), t).start()

    def second_half(t):
        arrive_halo(ascending, t)
        sources(t, half, freq_group)
        ret_copy(near_side, t).start()
        ret_local(t).start()

    first_half(0)
    for t in range(1, parts):
        for dy in range(1, sides):
            arrive_group(dy, t)
        first_half(t)
        second_half(t - 1)
    second_half(parts - 1)

    sum_out[...] = jnp.sum(acc[...], axis=0, keepdims=True)

    def sum_copy(step):
        return remote(
            sum_out, sum_in.at[me], sum_send.at[step - 1], sum_recv.at[me], (me + step) % count
        )

    for step in range(1, count):
        sum_copy(step).start()
    sum_in[me] = sum_out[...]
    for step in range(1, count):
        source = (me + step) % count
        remote(
            sum_out, sum_in.at[source], sum_send.at[0], sum_recv.at[source], source
        ).wait_recv()

    per_row = count // group
    mine_row = me // per_row
    height_sum = jnp.zeros((1, width), f32)
    mine = jnp.zeros((1, width), f32)
    for g in range(group):
        mass = sum_in[g]
        for other in range(1, zones):
            mass = mass + sum_in[other * group + g]
        sea_row = aux_ref[0:1, g * width : (g + 1) * width]
        height = sea_row * (4.0 * jnp.sqrt(mass * (1.0 / (NF * ND)) + 1e-06))
        height_sum = height_sum + height
        mine = jnp.where(mine_row == g, height, mine)
    points = cells // count
    shift = (me % per_row) * points
    turned = pltpu.roll(jnp.broadcast_to(mine, (8, width)), (width - shift) % width, 1)
    wave_ref[...] = turned[0, :points]
    mean_ref[...] = jnp.sum(height_sum, axis=1, keepdims=True) * (1.0 / (SEA_DEV * count))

    for t in range(parts):
        for i in range(1, group):
            peer = rank_of(offsets[i])
            remote(
                done.at[pl.ds(0, freq_dev), :, lanes_of(t)], out_ref.at[:, :, tile_of(peer, t)],
                ret_send.at[peer, t], ret_recv.at[peer, t], zone * group + peer,
            ).wait_recv()
            for f in range(freq_dev):
                y_copy(f, i, t).wait_send()
            ret_copy(peer, t).wait_send()
        ret_local(t).wait()
    for step in range(1, count):
        remote(
            mom_out.at[:, cells_of(0)], mom_in.at[me], mom_send.at[step - 1],
            mom_recv.at[me], (me + step) % count,
        ).wait_send()
        sum_copy(step).wait_send()

    @pl.when(zone < zones - 1)
    def _():
        for t in range(parts):
            for slot in range(freq_group - HALO, freq_group):
                up_copy(slot, t).wait_send()

    @pl.when(zone > 0)
    def _():
        for t in range(parts):
            for slot in range(HALO):
                down_copy(slot, t).wait_send()


def store_kernel(new_in, wave_in, new_out, wave_out, sem):
    copies = [
        pltpu.make_async_copy(new_in, new_out, sem.at[0]),
        pltpu.make_async_copy(wave_in, wave_out, sem.at[1]),
    ]
    for copy in copies:
        copy.start()
    for copy in copies:
        copy.wait()


def fused_local(spectrum, sea_mask, wind_speed, wind_angle):
    count = lax.axis_size("spec")
    bins_dev, cells = spectrum.shape
    group = group_size(count, bins_dev, cells)
    freq_dev = bins_dev // ND
    freq_group = freq_dev * group
    width = cells // group
    points = cells // count
    parts = width // LANES
    f32 = jnp.float32
    dma = pltpu.SemaphoreType.DMA
    out, wave, mean = pl.pallas_call(
        functools.partial(fused_kernel, count, group),
        out_shape=(
            pltpu.VMEM((freq_dev, ND, cells), f32),
            pltpu.VMEM((points,), f32),
            jax.ShapeDtypeStruct((1, 1), f32),
        ),
        in_specs=[
            pl.BlockSpec(memory_space=pl.ANY),
        ]
        * 4,
        out_specs=(
            pl.BlockSpec(memory_space=pltpu.VMEM),
            pl.BlockSpec(memory_space=pltpu.VMEM),
            pl.BlockSpec(memory_space=pltpu.VMEM),
        ),
        scratch_shapes=[
            pltpu.VMEM((cells,), jnp.int32),
            pltpu.VMEM((cells,), f32),
            pltpu.VMEM((cells,), f32),
            pltpu.VMEM((1, cells), f32),
            dma((3,)),
            pltpu.VMEM((bins_dev, cells), f32),
            pltpu.VMEM((freq_dev, ND, cells), f32),
            pltpu.VMEM((freq_group + 2 * HALO, ND, width), f32),
            pltpu.VMEM((freq_group, ND, width), f32),
            pltpu.VMEM((2, cells), f32),
            pltpu.VMEM((count, 2, width), f32),
            pltpu.VMEM((ND, width), f32),
            pltpu.VMEM((ND, width), f32),
            pltpu.VMEM((1, width), f32),
            pltpu.VMEM((count, 1, width), f32),
            dma((freq_dev,)),
            dma((freq_group + 2 * HALO, parts)),
            dma((group - 1, freq_dev, parts)),
            dma((HALO, parts)),
            dma((HALO, parts)),
            dma((count - 1,)),
            dma((count,)),
            dma((group, parts)),
            dma((group, parts)),
            dma((count - 1,)),
            dma((count,)),
        ],
        compiler_params=pltpu.CompilerParams(collective_id=0, has_side_effects=True),
    )(sea_mask, wind_speed, wind_angle, spectrum)
    out, wave = pl.pallas_call(
        store_kernel,
        out_shape=(
            pltpu.HBM(out.shape, f32),
            pltpu.HBM(wave.shape, f32),
        ),
        in_specs=[pl.BlockSpec(memory_space=pltpu.VMEM)] * 2,
        out_specs=(pl.BlockSpec(memory_space=pltpu.HBM),) * 2,
        scratch_shapes=[dma((2,))],
    )(
        pltpu.with_memory_space_constraint(out, pltpu.VMEM),
        pltpu.with_memory_space_constraint(wave, pltpu.VMEM),
    )
    return (out.reshape(bins_dev, cells), wave, mean.reshape(1))


def solution(mesh):
    in_specs = (P(("grp", "spec"), None), P(), P("grp"), P("grp"))
    out_specs = (P(("grp", "spec"), None), P(("grp", "spec")), P("grp"))

    def body(spectrum, sea_mask, wind_speed, wind_angle):
        fits = group_size(mesh.shape["spec"], *spectrum.shape)
        plan = fused_local if fits else local
        return plan(spectrum, sea_mask, wind_speed, wind_angle)

    return jax.shard_map(body, mesh=mesh, in_specs=in_specs, out_specs=out_specs, check_vma=False)
```
